8 devices in a mesh: dp: 1 (over z), tp: 8 (over y, x, core).
Axes of the slice: x: 2, y: 2, z: 1, core: 2. Of those that a mesh axis runs over, the one named last changes fastest.
Arguments:
- tok_hidden: bfloat16 [16, 4096], P('dp')
- seq_lens: int32 [16], P('dp')
- k_cache: bfloat16 [16, 512, 8, 128], P('dp', None, 'tp')
- v_cache: bfloat16 [16, 512, 8, 128], P('dp', None, 'tp')
- next_tok: int32 [16], P('dp')
- g_attn: bfloat16 [4096], replicated
- w_q: bfloat16 [4096, 4096], P(None, 'tp')
- b_q: bfloat16 [4096], P('tp')
- w_k: bfloat16 [4096, 1024], P(None, 'tp')
- b_k: bfloat16 [1024], P('tp')
- w_v: bfloat16 [4096, 1024], P(None, 'tp')
- b_v: bfloat16 [1024], P('tp')
- w_o: bfloat16 [4096, 4096], P('tp')
- g_mlp: bfloat16 [4096], replicated
- w_gate: bfloat16 [4096, 14336], P(None, 'tp')
- w_up: bfloat16 [4096, 14336], P(None, 'tp')
- w_down: bfloat16 [14336, 4096], P('tp')
- g_final: bfloat16 [4096], replicated
- w_head: bfloat16 [128256, 4096], P('tp')
Outputs:
- output 1: bfloat16 [16, 4096], P('dp')
- output 2: bfloat16 [16, 512, 8, 128], P('dp', None, 'tp')
- output 3: bfloat16 [16, 512, 8, 128], P('dp', None, 'tp')
- output 4: float32 [16], P('dp')
- output 5: float32 [16], P('dp')
All inputs are finite; a program needn't handle non-finite values.
Results may differ from the reference program's by a relative error of at most 0.0134601.
Values are sent between devices in bfloat16 or wider.
A program may use at most 1 GiB of HBM per device.

```python
import math
import jax
import jax.numpy as jnp
from jax import lax

BATCH = 16
LMAX = 512
D = 4096
HEADS = 32
KV_HEADS = 8
HEAD = 128
FF = 14336
VOCAB = 128256
KV_SLOTS = 8
THETA = 1000000
EPS = 1e-6
COPIES = KV_SLOTS // KV_HEADS
GROUP = HEADS // KV_SLOTS


def rms_norm(values, gain_vec):
    vals_f32 = values.astype(jnp.float32)
    inv_rms = lax.rsqrt(jnp.mean(vals_f32 * vals_f32, axis=-1, keepdims=True) + EPS)
    return (vals_f32 * inv_rms * gain_vec.astype(jnp.float32)).astype(jnp.bfloat16)


def rotary(values, positions):
    half_dim = values.shape[-1] // 2
    inv_freq = jnp.power(float(THETA), jnp.arange(half_dim, dtype=jnp.float32) * (-2.0 / values.shape[-1]))
    angles = positions.astype(jnp.float32)[:, None] * inv_freq[None, :]
    cos_part = jnp.cos(angles)[:, None, :]
    sin_part = jnp.sin(angles)[:, None, :]
    first_half = values[..., :half_dim]
    second_half = values[..., half_dim:]
    return jnp.concatenate([first_half * cos_part - second_half * sin_part, second_half * cos_part + first_half * sin_part], axis=-1)


def draw_lengths(len_key):
    exp_key, off_key, pick_key = jax.random.split(len_key, 3)
    log_max = int(math.log2(LMAX))
    exponent = jax.random.randint(exp_key, (BATCH,), 0, log_max)
    base_len = jnp.left_shift(jnp.ones((BATCH,), jnp.int32), exponent)
    offset = jax.random.randint(off_key, (BATCH,), 0, LMAX) % base_len
    longest = jax.random.randint(pick_key, (), 0, BATCH)
    return jnp.where(jnp.arange(BATCH) == longest, LMAX - 1, base_len + offset).astype(jnp.int32)


def gaussian(rand_key, arr_shape, spread):
    return jax.random.normal(rand_key, arr_shape, jnp.float32) * spread


def setup_inputs(seed: int = 0, part: int = 0) -> dict:
    shared_keys = jax.random.split(jax.random.key(seed), 16)
    part_keys = jax.random.split(jax.random.fold_in(jax.random.key(seed + 1), part), 8)
    k_scale = math.sqrt(max(math.log(LMAX / 8.0), 1.0) / 1.25)
    k_base = gaussian(part_keys[2], (BATCH, LMAX, KV_HEADS, HEAD), k_scale)
    v_base = gaussian(part_keys[3], (BATCH, LMAX, KV_HEADS, HEAD), 1.0)
    w_k = gaussian(shared_keys[3], (D, KV_HEADS, HEAD), D ** -0.5)
    b_k = gaussian(shared_keys[4], (KV_HEADS, HEAD), 0.5)
    w_v = gaussian(shared_keys[5], (D, KV_HEADS, HEAD), D ** -0.5)
    b_v = gaussian(shared_keys[6], (KV_HEADS, HEAD), 0.5)
    return {
        'tok_hidden': gaussian(part_keys[0], (BATCH, D), 1.0).astype(jnp.bfloat16),
        'seq_lens': draw_lengths(part_keys[1]),
        'k_cache': jnp.repeat(k_base, COPIES, axis=2).astype(jnp.bfloat16),
        'v_cache': jnp.repeat(v_base, COPIES, axis=2).astype(jnp.bfloat16),
        'next_tok': jax.random.randint(part_keys[4], (BATCH,), 0, VOCAB),
        'g_attn': (1.0 + gaussian(shared_keys[0], (D,), 0.2)).astype(jnp.bfloat16),
        'w_q': gaussian(shared_keys[1], (D, HEADS * HEAD), D ** -0.5).astype(jnp.bfloat16),
        'b_q': gaussian(shared_keys[2], (HEADS * HEAD,), 0.5).astype(jnp.bfloat16),
        'w_k': jnp.repeat(w_k, COPIES, axis=1).reshape(D, KV_SLOTS * HEAD).astype(jnp.bfloat16),
        'b_k': jnp.repeat(b_k, COPIES, axis=0).reshape(KV_SLOTS * HEAD).astype(jnp.bfloat16),
        'w_v': jnp.repeat(w_v, COPIES, axis=1).reshape(D, KV_SLOTS * HEAD).astype(jnp.bfloat16),
        'b_v': jnp.repeat(b_v, COPIES, axis=0).reshape(KV_SLOTS * HEAD).astype(jnp.bfloat16),
        'w_o': gaussian(shared_keys[7], (HEADS * HEAD, D), (HEADS * HEAD) ** -0.5).astype(jnp.bfloat16),
        'g_mlp': (1.0 + gaussian(shared_keys[8], (D,), 0.2)).astype(jnp.bfloat16),
        'w_gate': gaussian(shared_keys[9], (D, FF), D ** -0.5).astype(jnp.bfloat16),
        'w_up': gaussian(shared_keys[10], (D, FF), D ** -0.5).astype(jnp.bfloat16),
        'w_down': gaussian(shared_keys[11], (FF, D), FF ** -0.5).astype(jnp.bfloat16),
        'g_final': (3.0 + gaussian(shared_keys[12], (D,), 0.5)).astype(jnp.bfloat16),
        'w_head': gaussian(shared_keys[13], (VOCAB, D), D ** -0.5).astype(jnp.bfloat16),
    }


def reference(tok_hidden, seq_lens, k_cache, v_cache, next_tok, g_attn, w_q, b_q, w_k, b_k, w_v, b_v, w_o, g_mlp, w_gate, w_up, w_down, g_final, w_head):
    normed = rms_norm(tok_hidden, g_attn)
    q_proj = jnp.dot(normed, w_q, preferred_element_type=jnp.float32) + b_q.astype(jnp.float32)
    k_proj = jnp.dot(normed, w_k, preferred_element_type=jnp.float32) + b_k.astype(jnp.float32)
    v_proj = jnp.dot(normed, w_v, preferred_element_type=jnp.float32) + b_v.astype(jnp.float32)
    q_rot = rotary(q_proj.reshape(BATCH, HEADS, HEAD), seq_lens).astype(jnp.bfloat16)
    k_new = rotary(k_proj.reshape(BATCH, KV_SLOTS, HEAD), seq_lens).astype(jnp.bfloat16)
    v_new = v_proj.reshape(BATCH, KV_SLOTS, HEAD).astype(jnp.bfloat16)
    slot_ids = jnp.arange(LMAX)
    write_mask = (slot_ids[None, :] == seq_lens[:, None])[:, :, None, None]
    k_all = jnp.where(write_mask, k_new[:, None], k_cache)
    v_all = jnp.where(write_mask, v_new[:, None], v_cache)

    def one_row(row_args):
        q_row, k_row, v_row, length = row_args
        q_grp = q_row.reshape(KV_SLOTS, GROUP, HEAD).astype(jnp.float32)
        scores = jnp.einsum('kgd,lkd->kgl', q_grp, k_row.astype(jnp.float32)) * (HEAD ** -0.5)
        scores = jnp.where((slot_ids <= length)[None, None, :], scores, -jnp.inf)
        attn_probs = jax.nn.softmax(scores, axis=-1).astype(jnp.bfloat16).astype(jnp.float32)
        attn_vals = jnp.einsum('kgl,lkd->kgd', attn_probs, v_row.astype(jnp.float32))
        return attn_vals.reshape(HEADS * HEAD).astype(jnp.bfloat16)

    attn_out = lax.map(one_row, (q_rot, k_all, v_all, seq_lens))
    attn_proj = jnp.dot(attn_out, w_o, preferred_element_type=jnp.float32)
    residual = (tok_hidden.astype(jnp.float32) + attn_proj).astype(jnp.bfloat16)
    mlp_in = rms_norm(residual, g_mlp)
    gate_proj = jnp.dot(mlp_in, w_gate, preferred_element_type=jnp.float32)
    up_proj = jnp.dot(mlp_in, w_up, preferred_element_type=jnp.float32)
    hidden = (jax.nn.silu(gate_proj) * up_proj).astype(jnp.bfloat16)
    down_proj = jnp.dot(hidden, w_down, preferred_element_type=jnp.float32)
    y_out = (residual.astype(jnp.float32) + down_proj).astype(jnp.bfloat16)
    final_norm = rms_norm(y_out, g_final)
    logits = lax.dot_general(final_norm, w_head, (((1,), (1,)), ((), ())), preferred_element_type=jnp.float32)
    norm_lse = jax.nn.logsumexp(logits, axis=-1)
    vocab_ids = jnp.arange(VOCAB)
    target = jnp.sum(jnp.where(vocab_ids[None, :] == next_tok[:, None], logits, 0.0), axis=-1)
    tok_logp = target - norm_lse
    return (y_out, k_all, v_all, tok_logp, norm_lse)
```

```python
import functools

import jax
import jax.numpy as jnp
import numpy as np
from jax import lax
from jax.experimental import pallas as pl
from jax.experimental.pallas import tpu as pltpu
from jax.sharding import PartitionSpec as P

THETA = 1000000.0
EPS = 1e-6
F32 = jnp.float32
BF16 = jnp.bfloat16
ROWS = 16
D = 4096
HD = 128
GROUP = 4
LMAX = 512
FF = 1792
VOC = 16032
COL = 512
NDEV = 8
SLOTS = 14
CHUNK = 512
NFULL = VOC // CHUNK
TAIL = VOC - NFULL * CHUNK
VMEM_CAP = 64 * 2**20 - 65536

NT_DIMS = (((1,), (1,)), ((), ()))
NN_DIMS = (((1,), (0,)), ((), ()))


def mm(lhs, rhs, dims=NN_DIMS):
    return lax.dot_general(lhs, rhs, dims, preferred_element_type=F32)


def row_vector(scalars_ref, dtype, shape, axis):
    ids = lax.broadcasted_iota(jnp.int32, shape, axis)
    vec = jnp.zeros(shape, dtype)
    for row in range(ROWS):
        vec = jnp.where(ids == row, scalars_ref[row].astype(dtype), vec)
    return vec


def attn_kernel(lens_ref, x_hbm, g_ref, freq_ref, bq_ref, bk_ref, bv_ref, wq_hbm, wk_hbm, wv_hbm, kc_hbm, vc_hbm,
                ko_hbm, vo_hbm, o_ref,
                x_buf, wq, wk, wv, kbuf, vbuf, q_scr, s_scr, o_scr, sems, out_sems):
    quarter = D // 4
    bq = ROWS // 4
    copies = [pltpu.make_async_copy(x_hbm, x_buf, sems.at[0]),
              pltpu.make_async_copy(wk_hbm, wk, sems.at[1]),
              pltpu.make_async_copy(wv_hbm, wv, sems.at[2]),
              pltpu.make_async_copy(wq_hbm, wq, sems.at[3]),
              pltpu.make_async_copy(kc_hbm, kbuf, sems.at[4]),
              pltpu.make_async_copy(vc_hbm, vbuf, sems.at[5])]
    for cp in copies:
        cp.start()
    pos = row_vector(lens_ref, F32, (ROWS, HD), 0)
    angles = pos * freq_ref[...]
    cos = jnp.cos(angles)
    lane = lax.broadcasted_iota(jnp.int32, (ROWS, HD), 1)
    sin = jnp.where(lane < HD // 2, -jnp.sin(angles), jnp.sin(angles))
    copies[0].wait()
    xf = x_buf[...].astype(F32)
    inv = lax.rsqrt(jnp.mean(xf * xf, axis=-1, keepdims=True) + EPS)
    normed = (xf * inv * g_ref[...].astype(F32)).astype(BF16)
    copies[1].wait()
    k_proj = mm(normed, wk[...]) + bk_ref[...].astype(F32)
    k_new = (k_proj * cos + pltpu.roll(k_proj, HD // 2, 1) * sin).astype(BF16).astype(F32)
    copies[2].wait()
    v_new = (mm(normed, wv[...]) + bv_ref[...].astype(F32)).astype(BF16).astype(F32)
    copies[3].wait()
    q_proj = mm(normed, wq[...]) + bq_ref[...].astype(F32)
    for h in range(GROUP):
        q_h = q_proj[:, h * HD:(h + 1) * HD]
        q_scr[:, h, :] = q_h * cos + pltpu.roll(q_h, HD // 2, 1) * sin
    sub = lax.broadcasted_iota(jnp.int32, (16, HD), 0)

    def insert(buf, b, new):
        at = lens_ref[b]
        base = pl.multiple_of((at // 16) * 16, 16)
        block = buf[b, pl.ds(base, 16), :].astype(F32)
        fresh = jnp.broadcast_to(new[b:b + 1, :], (16, HD))
        buf[b, pl.ds(base, 16), :] = jnp.where(sub == at - base, fresh, block).astype(BF16)

    copies[4].wait()
    for b in range(ROWS):
        insert(kbuf, b, k_new)
    slot_ids = lax.broadcasted_iota(jnp.int32, (GROUP, LMAX), 1)
    for b in range(ROWS):
        s_b = mm(q_scr[b].astype(BF16), kbuf[b], NT_DIMS) * (HD ** -0.5)
        s_scr[b] = jnp.where(slot_ids <= lens_ref[b], s_b, -jnp.inf)
    k_out = pltpu.make_async_copy(kbuf, ko_hbm, out_sems.at[0])
    k_out.start()
    copies[5].wait()
    for b in range(ROWS):
        insert(vbuf, b, v_new)
    scores = s_scr[...]
    e = jnp.exp(scores - jnp.max(scores, axis=-1, keepdims=True))
    s_scr[...] = e / jnp.sum(e, axis=-1, keepdims=True)
    for b in range(ROWS):
        o_scr[b] = mm(s_scr[b].astype(BF16), vbuf[b])
    v_out = pltpu.make_async_copy(vbuf, vo_hbm, out_sems.at[1])
    v_out.start()
    for h in range(GROUP):
        o_ref[:, h * HD:(h + 1) * HD] = o_scr[:, h, :].astype(BF16)
    k_out.wait()
    v_out.wait()


def flip(me, k):
    out = 0
    for bit in (1, 2, 4):
        mine = lax.rem(me // bit, 2)
        out = out + bit * ((1 - mine) if k & bit else mine)
    return out


def norm_cols(parts_ref, g_ref, out_ref):
    total = jnp.zeros((ROWS, 1), F32)
    for j in range(NDEV):
        part = parts_ref[j].astype(F32)
        total = total + jnp.sum(part * part, axis=-1, keepdims=True)
    inv = lax.rsqrt(total * (1.0 / D) + EPS)
    for j in range(NDEV):
        cols = slice(j * COL, (j + 1) * COL)
        out_ref[:, cols] = (parts_ref[j].astype(F32) * inv * g_ref[:, cols].astype(F32)).astype(BF16)


def step_kernel(tok_ref, x_ref, o_ref, gm_ref, gf_ref, wo_hbm, wg_hbm, wu_hbm, wd_hbm, wh_hbm,
                y_hbm, st_ref,
                ring, mbuf, gacc, uacc, hbuf, zbuf, rs_send, rs_recv, own, gath, st_send, st_recv,
                ring_sems, rs_ssem, rs_rsem, ag_ssem, ag_rsem, st_ssem, st_rsem, y_sem):
    me = lax.axis_index('tp')
    peers = {k: flip(me, k) for k in range(1, NDEV)}
    order = (7, 6, 5, 4, 3, 2, 1)

    def fetch(c):
        slot, sem = ring.at[c % SLOTS], ring_sems.at[c % SLOTS]
        if c == 0:
            return [pltpu.make_async_copy(wo_hbm, slot, sem)]
        if c <= 8:
            rows = pl.ds((c - 1) * CHUNK, CHUNK)
            return [pltpu.make_async_copy(wg_hbm.at[rows, :], slot.at[:, 0:FF], sem),
                    pltpu.make_async_copy(wu_hbm.at[rows, :], slot.at[:, FF:2 * FF], ring_sems.at[SLOTS + c - 1])]
        first = (c - 9) * CHUNK
        size = min(CHUNK, FF - first)
        return [pltpu.make_async_copy(wd_hbm.at[pl.ds(first, size), :], slot.at[0:size, :], sem)]

    def head_copy(h, size=CHUNK):
        slot = lax.rem(h + 13, SLOTS)
        return pltpu.make_async_copy(wh_hbm.at[pl.ds(pl.multiple_of(h * CHUNK, CHUNK), size), :],
                                     ring.at[slot, 0:size, :], ring_sems.at[slot])

    for c in range(13):
        for cp in fetch(c):
            cp.start()
    head_copy(0).start()
    barrier = pltpu.get_barrier_semaphore()
    for k in order:
        pl.semaphore_signal(barrier, inc=1, device_id={'tp': peers[k]}, device_id_type=pl.DeviceIdType.MESH)
    pl.semaphore_wait(barrier, NDEV - 1)

    def remote(src, dst, ssem, rsem, k):
        return pltpu.make_async_remote_copy(src_ref=src, dst_ref=dst, send_sem=ssem, recv_sem=rsem,
                                            device_id={'tp': peers[k]}, device_id_type=pl.DeviceIdType.MESH)

    sends = []

    def all_reduce(phase, partial, residual):
        copies = {}
        for k in order:
            rs_send[phase, k] = partial(peers[k]).astype(BF16)
            copies[k] = remote(rs_send.at[phase, k], rs_recv.at[phase, k], rs_ssem.at[phase, k], rs_rsem.at[phase, k], k)
            copies[k].start()
            sends.append(copies[k])
        total = partial(me)
        for k in reversed(order):
            copies[k].wait_recv()
            total = total + rs_recv[phase, k].astype(F32)
        mine = (residual.astype(F32) + total).astype(BF16)
        own[phase] = mine
        gath[phase, me] = mine
        copies = {}
        for k in order:
            copies[k] = remote(own.at[phase], gath.at[phase, me], ag_ssem.at[phase, k], ag_rsem.at[phase, k], k)
            copies[k].start()
            sends.append(copies[k])
        for k in reversed(order):
            copies[k].wait_recv()

    def columns(dev):
        return pl.ds(pl.multiple_of(dev * COL, COL), COL)

    fetch(0)[0].wait()
    all_reduce(0, lambda dev: mm(o_ref[...], ring[0, :, columns(dev)]), x_ref[:, columns(me)])
    head_copy(1).start()
    norm_cols(gath.at[0], gm_ref, mbuf)

    for j in range(8):
        for cp in fetch(1 + j):
            cp.wait()
        m_j = mbuf[:, j * CHUNK:(j + 1) * CHUNK]
        g_j = mm(m_j, ring[1 + j, :, 0:FF])
        u_j = mm(m_j, ring[1 + j, :, FF:2 * FF])
        if j == 0:
            gacc[...] = g_j
            uacc[...] = u_j
        else:
            gacc[...] += g_j
            uacc[...] += u_j
        head_copy(2 + j).start()
    gate = gacc[...]
    hbuf[...] = (gate * jax.nn.sigmoid(gate) * uacc[...]).astype(BF16)

    for c in range(9, 13):
        fetch(c)[0].wait()

    def down(dev):
        total = jnp.zeros((ROWS, COL), F32)
        for j in range(4):
            first, size = j * CHUNK, min(CHUNK, FF - j * CHUNK)
            total = total + mm(hbuf[:, first:first + size], ring[9 + j, 0:size, columns(dev)])
        return total

    all_reduce(1, down, own[0])
    for h in range(10, 14):
        head_copy(h).start()
    y_copies = [pltpu.make_async_copy(gath.at[1, j], y_hbm.at[:, j * COL:(j + 1) * COL], y_sem.at[j]) for j in range(NDEV)]
    for cp in y_copies:
        cp.start()
    norm_cols(gath.at[1], gf_ref, mbuf)

    target = row_vector(tok_ref, jnp.int32, (1, ROWS), 1) - me * VOC

    def stats(z, first, carry):
        top, acc, hit = carry
        ids = lax.broadcasted_iota(jnp.int32, z.shape, 0) + first
        new_top = jnp.maximum(top, jnp.max(z, axis=0, keepdims=True))
        acc = acc * jnp.exp(top - new_top) + jnp.sum(jnp.exp(z - new_top), axis=0, keepdims=True)
        hit = hit + jnp.sum(jnp.where(ids == target, z, 0.0), axis=0, keepdims=True)
        return new_top, acc, hit

    def score(h, size=CHUNK):
        return mm(ring[lax.rem(h + 13, SLOTS), 0:size, :], mbuf[...], NT_DIMS)

    def refill(h):
        @pl.when(h + SLOTS < NFULL)
        def _():
            head_copy(h + SLOTS).start()

        @pl.when(h + SLOTS == NFULL)
        def _():
            head_copy(NFULL, TAIL).start()

    carry = (jnp.full((1, ROWS), -jnp.inf, F32), jnp.zeros((1, ROWS), F32), jnp.zeros((1, ROWS), F32))

    def pair(i, carry, first):
        h = 2 * i
        head_copy(h).wait()
        head_copy(h + 1).wait()
        now = lax.rem(i, 2)
        z0 = score(h)
        z1 = score(h + 1)
        if not first:
            carry = stats(zbuf[1 - now], (h - 2) * CHUNK, carry)
        zbuf[now, 0:CHUNK, :] = z0
        zbuf[now, CHUNK:, :] = z1
        refill(h)
        refill(h + 1)
        return carry

    pairs = NFULL // 2
    carry = pair(0, carry, True)
    carry = lax.fori_loop(1, pairs, lambda i, c: pair(i, c, False), carry)
    head_copy(NFULL - 1).wait()
    z_last = score(NFULL - 1)
    carry = stats(zbuf[(pairs - 1) % 2], (pairs - 1) * 2 * CHUNK, carry)
    carry = stats(z_last, (NFULL - 1) * CHUNK, carry)
    head_copy(NFULL, TAIL).wait()
    carry = stats(score(NFULL, TAIL), NFULL * CHUNK, carry)

    top, acc, hit = carry
    st_send[0:1, 0:ROWS] = top
    st_send[1:2, 0:ROWS] = acc
    st_send[2:3, 0:ROWS] = hit
    copies = {}
    for k in order:
        copies[k] = remote(st_send, st_recv.at[k], st_ssem.at[k], st_rsem.at[k], k)
        copies[k].start()
        sends.append(copies[k])
    for k in reversed(order):
        copies[k].wait_recv()
    tops, accs, hits = [top], [acc], [hit]
    for k in reversed(order):
        tops.append(st_recv[k, 0:1, 0:ROWS])
        accs.append(st_recv[k, 1:2, 0:ROWS])
        hits.append(st_recv[k, 2:3, 0:ROWS])
    best = functools.reduce(jnp.maximum, tops)
    exp_sum = sum(a * jnp.exp(t - best) for t, a in zip(tops, accs))
    lse = best + jnp.log(exp_sum)
    st_ref[0:1, 0:ROWS] = sum(hits) - lse
    st_ref[1:2, 0:ROWS] = lse
    for cp in sends:
        cp.wait_send()
    for cp in y_copies:
        cp.wait()


def rotary_freqs():
    half = HD // 2
    freq = np.power(THETA, np.arange(half) * (-2.0 / HD)).astype(np.float32)
    return np.concatenate([freq, freq])[None, :]


VM = pl.BlockSpec(memory_space=pltpu.VMEM)
SM = pl.BlockSpec(memory_space=pltpu.SMEM)
HB = pl.BlockSpec(memory_space=pl.ANY)
DMA = pltpu.SemaphoreType.DMA


def local_step(tok_hidden, seq_lens, k_cache, v_cache, next_tok, g_attn, w_q, b_q, w_k, b_k, w_v, b_v, w_o, g_mlp, w_gate, w_up, w_down, g_final, w_head):
    cache = jax.ShapeDtypeStruct((ROWS, LMAX, HD), BF16)
    k_out, v_out, attn_out = pl.pallas_call(
        attn_kernel,
        out_shape=(cache, cache, jax.ShapeDtypeStruct((ROWS, GROUP * HD), BF16)),
        in_specs=[SM, HB, VM, VM, VM, VM, VM, HB, HB, HB, HB, HB],
        out_specs=(HB, HB, VM),
        scratch_shapes=[
            pltpu.VMEM((ROWS, D), BF16),
            pltpu.VMEM((D, GROUP * HD), BF16),
            pltpu.VMEM((D, HD), BF16),
            pltpu.VMEM((D, HD), BF16),
            pltpu.VMEM((ROWS, LMAX, HD), BF16),
            pltpu.VMEM((ROWS, LMAX, HD), BF16),
            pltpu.VMEM((ROWS, GROUP, HD), F32),
            pltpu.VMEM((ROWS, GROUP, LMAX), F32),
            pltpu.VMEM((ROWS, GROUP, HD), F32),
            DMA((6,)),
            DMA((2,)),
        ],
        compiler_params=pltpu.CompilerParams(vmem_limit_bytes=48 * 2**20),
        name='attn',
    )(seq_lens, tok_hidden, g_attn[None], jnp.asarray(rotary_freqs()), b_q[None], b_k[None], b_v[None], w_q, w_k, w_v,
      k_cache.reshape(ROWS, LMAX, HD), v_cache.reshape(ROWS, LMAX, HD))
    y_out, stats = pl.pallas_call(
        step_kernel,
        out_shape=(jax.ShapeDtypeStruct((ROWS, D), BF16), jax.ShapeDtypeStruct((8, 128), F32)),
        in_specs=[SM, VM, VM, VM, VM, HB, HB, HB, HB, HB],
        out_specs=(HB, VM),
        scratch_shapes=[
            pltpu.VMEM((SLOTS, CHUNK, D), BF16),
            pltpu.VMEM((ROWS, D), BF16),
            pltpu.VMEM((ROWS, FF), F32),
            pltpu.VMEM((ROWS, FF), F32),
            pltpu.VMEM((ROWS, FF), BF16),
            pltpu.VMEM((2, 2 * CHUNK, ROWS), F32),
            pltpu.VMEM((2, NDEV, ROWS, COL), BF16),
            pltpu.VMEM((2, NDEV, ROWS, COL), BF16),
            pltpu.VMEM((2, ROWS, COL), BF16),
            pltpu.VMEM((2, NDEV, ROWS, COL), BF16),
            pltpu.VMEM((8, 128), F32),
            pltpu.VMEM((NDEV, 8, 128), F32),
            DMA((SLOTS + 8,)),
            DMA((2, NDEV)),
            DMA((2, NDEV)),
            DMA((2, NDEV)),
            DMA((2, NDEV)),
            DMA((NDEV,)),
            DMA((NDEV,)),
            DMA((NDEV,)),
        ],
        compiler_params=pltpu.CompilerParams(collective_id=0, has_side_effects=True, vmem_limit_bytes=VMEM_CAP),
        name='step',
    )(next_tok, tok_hidden, attn_out, g_mlp[None], g_final[None], w_o, w_gate, w_up, w_down, w_head)
    shape = (ROWS, LMAX, 1, HD)
    return y_out, k_out.reshape(shape), v_out.reshape(shape), stats[0, 0:ROWS], stats[1, 0:ROWS]


def solution(mesh):
    row_spec = P('dp', None)
    vec_spec = P('dp')
    cache_spec = P('dp', None, 'tp', None)
    col_spec = P(None, 'tp')
    part_spec = P('tp')
    whole_spec = P(None)
    in_specs = (row_spec, vec_spec, cache_spec, cache_spec, vec_spec, whole_spec, col_spec, part_spec, col_spec, part_spec, col_spec, part_spec, P('tp', None), whole_spec, col_spec, col_spec, P('tp', None), whole_spec, P('tp', None))
    out_specs = (row_spec, cache_spec, cache_spec, vec_spec, vec_spec)
    return jax.shard_map(local_step, mesh=mesh, in_specs=in_specs, out_specs=out_specs, check_vma=False)
```

```python
import functools

import jax
import jax.numpy as jnp
import numpy as np
from jax import lax
from jax.experimental import pallas as pl
from jax.experimental.pallas import tpu as pltpu
from jax.sharding import PartitionSpec as P

THETA = 1000000.0
EPS = 1e-6
F32 = jnp.float32
BF16 = jnp.bfloat16
ROWS = 16
D = 4096
HD = 128
GROUP = 4
LMAX = 512
FF = 1792
VOC = 16032
COL = 512
NDEV = 8
SLOTS = 11
CHUNK = 512
DEEP = 256
HEAD0 = 13
NFULL = VOC // CHUNK
TAIL = VOC - NFULL * CHUNK
PARTS = 4
VMEM_CAP = 64 * 2**20 - 65536

NT_DIMS = (((1,), (1,)), ((), ()))
NN_DIMS = (((1,), (0,)), ((), ()))


def mm(lhs, rhs, dims=NN_DIMS):
    return lax.dot_general(lhs, rhs, dims, preferred_element_type=F32)


def row_vector(scalars_ref, dtype, shape, axis):
    ids = lax.broadcasted_iota(jnp.int32, shape, axis)
    vec = jnp.zeros(shape, dtype)
    for row in range(ROWS):
        vec = jnp.where(ids == row, scalars_ref[row].astype(dtype), vec)
    return vec


def flip(me, k):
    out = 0
    for bit in (1, 2, 4):
        mine = lax.rem(me // bit, 2)
        out = out + bit * ((1 - mine) if k & bit else mine)
    return out


def norm_cols(parts_ref, gain, out_ref):
    total = jnp.zeros((ROWS, 1), F32)
    for j in range(NDEV):
        part = parts_ref[j].astype(F32)
        total = total + jnp.sum(part * part, axis=-1, keepdims=True)
    inv = lax.rsqrt(total * (1.0 / D) + EPS)
    for j in range(NDEV):
        cols = slice(j * COL, (j + 1) * COL)
        out_ref[:, cols] = (parts_ref[j].astype(F32) * inv * gain[:, cols]).astype(BF16)


def step_kernel(lens_ref, tok_ref, x_hbm, ga_hbm, gm_ref, gf_ref, freq_ref, bq_ref, bk_ref, bv_ref,
                wq_hbm, wk_hbm, wv_hbm, kc_hbm, vc_hbm, wo_hbm, wg_hbm, wu_hbm, wd_hbm, wh_hbm,
                y_hbm, kn_ref, vn_ref, st_ref,
                ring, x_buf, ga_buf, wq, wkv, kbuf, vbuf, q_scr, s_scr, o_scr, obuf,
                mbuf, gacc, uacc, hbuf, za_buf, zb_buf, rs_send, rs_recv, own, gath, st_send, st_recv,
                in_sems, ring_sems, rs_ssem, rs_rsem, ag_ssem, ag_rsem, st_ssem, st_rsem, y_sem):
    me = lax.axis_index('tp')
    peers = {k: flip(me, k) for k in range(1, NDEV)}
    order = (7, 6, 5, 4, 3, 2, 1)

    def fetch(c):
        slot, sem = ring.at[c % SLOTS], ring_sems.at[c % SLOTS]
        if c == 0:
            return [pltpu.make_async_copy(wo_hbm, slot, sem)]
        if c <= 8:
            rows = pl.ds((c - 1) * CHUNK, CHUNK)
            return [pltpu.make_async_copy(wg_hbm.at[rows, :], slot.at[:, 0:FF], sem),
                    pltpu.make_async_copy(wu_hbm.at[rows, :], slot.at[:, FF:2 * FF], ring_sems.at[SLOTS + c - 1])]
        first = (c - 9) * CHUNK
        size = min(CHUNK, FF - first)
        return [pltpu.make_async_copy(wd_hbm.at[pl.ds(first, size), :], slot.at[0:size, :], sem)]

    def head_slot(h):
        return lax.rem(h + HEAD0, SLOTS)

    def head_copy(h, size=CHUNK):
        slot = head_slot(h)
        return pltpu.make_async_copy(wh_hbm.at[pl.ds(pl.multiple_of(h * CHUNK, CHUNK), size), :],
                                     ring.at[slot, 0:size, :], ring_sems.at[slot])

    def start_chunk(c):
        for cp in (fetch(c) if c < HEAD0 else [head_copy(c - HEAD0)]):
            cp.start()

    x_copy = pltpu.make_async_copy(x_hbm, x_buf, in_sems.at[0])
    ga_copy = pltpu.make_async_copy(ga_hbm, ga_buf, in_sems.at[1])
    wk_copy = pltpu.make_async_copy(wk_hbm, wkv.at[:, 0:HD], in_sems.at[2])
    wv_copy = pltpu.make_async_copy(wv_hbm, wkv.at[:, HD:2 * HD], in_sems.at[3])
    wq_copy = pltpu.make_async_copy(wq_hbm, wq, in_sems.at[4])
    kc_copy = pltpu.make_async_copy(kc_hbm, kbuf, in_sems.at[5])
    vc_copy = pltpu.make_async_copy(vc_hbm, vbuf, in_sems.at[6])
    for cp in (x_copy, ga_copy, wq_copy, wk_copy, wv_copy, kc_copy, vc_copy):
        cp.start()
    for c in range(SLOTS):
        start_chunk(c)
    barrier = pltpu.get_barrier_semaphore()
    for k in order:
        pl.semaphore_signal(barrier, inc=1, device_id={'tp': peers[k]}, device_id_type=pl.DeviceIdType.MESH)

    angles = row_vector(lens_ref, F32, (ROWS, HD), 0) * freq_ref[...]
    cos = jnp.cos(angles)
    lane = lax.broadcasted_iota(jnp.int32, (ROWS, HD), 1)
    sin = jnp.sin(angles)
    sin = jnp.where(lane < HD // 2, -sin, sin)
    x_copy.wait()
    ga_copy.wait()
    xf = x_buf[...].astype(F32)
    inv = lax.rsqrt(jnp.mean(xf * xf, axis=-1, keepdims=True) + EPS)
    normed = (xf * inv * ga_buf[...].astype(F32)[None, :]).astype(BF16)
    wq_copy.wait()
    q_proj = mm(normed, wq[...]) + bq_ref[...].astype(F32)[None, :]
    for h in range(GROUP):
        q_h = q_proj[:, h * HD:(h + 1) * HD]
        q_scr[:, h, :] = (q_h * cos + pltpu.roll(q_h, HD // 2, 1) * sin).astype(BF16).astype(F32)
    wk_copy.wait()
    wv_copy.wait()
    kv_proj = mm(normed, wkv[...])
    k_proj = kv_proj[:, 0:HD] + bk_ref[...].astype(F32)[None, :]
    k_new = (k_proj * cos + pltpu.roll(k_proj, HD // 2, 1) * sin).astype(BF16)
    v_new = (kv_proj[:, HD:] + bv_ref[...].astype(F32)[None, :]).astype(BF16)
    kn_ref[...] = k_new
    vn_ref[...] = v_new

    kc_copy.wait()
    slot_ids = lax.broadcasted_iota(jnp.int32, (GROUP, LMAX), 1)
    for b in range(ROWS):
        s_b = mm(q_scr[b].astype(BF16), kbuf[b], NT_DIMS) * (HD ** -0.5)
        s_scr[b] = jnp.where(slot_ids < lens_ref[b], s_b, -jnp.inf)
    s_new = jnp.sum(q_scr[...] * k_new.astype(F32)[:, None, :], axis=-1, keepdims=True) * (HD ** -0.5)
    scores = s_scr[...]
    top = jnp.maximum(jnp.max(scores, axis=-1, keepdims=True), s_new)
    e = jnp.exp(scores - top)
    e_new = jnp.exp(s_new - top)
    denom = jnp.sum(e, axis=-1, keepdims=True) + e_new
    s_scr[...] = e / denom
    p_new = (e_new / denom).astype(BF16).astype(F32)
    vc_copy.wait()
    for b in range(ROWS):
        o_scr[b] = mm(s_scr[b].astype(BF16), vbuf[b])
    o_scr[...] += p_new * v_new.astype(F32)[:, None, :]
    for h in range(GROUP):
        obuf[:, h * HD:(h + 1) * HD] = o_scr[:, h, :].astype(BF16)

    pl.semaphore_wait(barrier, NDEV - 1)

    def remote(src, dst, ssem, rsem, k):
        return pltpu.make_async_remote_copy(src_ref=src, dst_ref=dst, send_sem=ssem, recv_sem=rsem,
                                            device_id={'tp': peers[k]}, device_id_type=pl.DeviceIdType.MESH)

    sends = []

    def all_reduce(phase, partial, residual):
        copies = {}
        for k in order:
            rs_send[phase, k] = partial(peers[k]).astype(BF16)
            copies[k] = remote(rs_send.at[phase, k], rs_recv.at[phase, k], rs_ssem.at[phase, k], rs_rsem.at[phase, k], k)
            copies[k].start()
            sends.append(copies[k])
        total = partial(me)
        for k in reversed(order):
            copies[k].wait_recv()
            total = total + rs_recv[phase, k].astype(F32)
        mine = (residual.astype(F32) + total).astype(BF16)
        own[phase] = mine
        gath[phase, me] = mine
        copies = {}
        for k in order:
            copies[k] = remote(own.at[phase], gath.at[phase, me], ag_ssem.at[phase, k], ag_rsem.at[phase, k], k)
            copies[k].start()
            sends.append(copies[k])
        for k in reversed(order):
            copies[k].wait_recv()

    def columns(dev):
        return pl.ds(pl.multiple_of(dev * COL, COL), COL)

    fetch(0)[0].wait()
    all_reduce(0, lambda dev: mm(obuf[...], ring[0, :, columns(dev)]), x_buf[:, columns(me)])
    start_chunk(SLOTS)
    norm_cols(gath.at[0], gm_ref[...].astype(F32)[None, :], mbuf)

    for j in range(8):
        for cp in fetch(1 + j):
            cp.wait()
        m_j = mbuf[:, j * CHUNK:(j + 1) * CHUNK]
        g_j = mm(m_j, ring[1 + j, :, 0:FF])
        u_j = mm(m_j, ring[1 + j, :, FF:2 * FF])
        if j == 0:
            gacc[...] = g_j
            uacc[...] = u_j
        else:
            gacc[...] += g_j
            uacc[...] += u_j
        start_chunk(1 + j + SLOTS)
    gate = gacc[...]
    hbuf[...] = (gate * jax.nn.sigmoid(gate) * uacc[...]).astype(BF16)

    for c in range(9, 13):
        fetch(c)[0].wait()

    def down(dev):
        total = jnp.zeros((ROWS, COL), F32)
        for j in range(4):
            first, size = j * CHUNK, min(CHUNK, FF - j * CHUNK)
            total = total + mm(hbuf[:, first:first + size], ring[(9 + j) % SLOTS, 0:size, columns(dev)])
        return total

    all_reduce(1, down, own[0])
    for c in range(9, 13):
        start_chunk(c + SLOTS)
    y_copies = [pltpu.make_async_copy(gath.at[1, j], y_hbm.at[:, j * COL:(j + 1) * COL], y_sem.at[j]) for j in range(NDEV)]
    for cp in y_copies:
        cp.start()
    norm_cols(gath.at[1], gf_ref[...].astype(F32)[None, :], mbuf)

    target_row = row_vector(tok_ref, jnp.int32, (1, ROWS), 1) - me * VOC
    target_col = row_vector(tok_ref, jnp.int32, (ROWS, 1), 0) - me * VOC

    def fold(carry, pieces, ids, target):
        top, acc, hit = carry
        new_top = functools.reduce(jnp.maximum, pieces, top)
        acc = acc * jnp.exp(top - new_top)
        for piece, at in zip(pieces, ids):
            acc = acc + jnp.exp(piece - new_top)
            hit = hit + jnp.where(at == target, piece, 0.0)
        return new_top, acc, hit

    def stats_a(z, first, carry):
        ids = lax.broadcasted_iota(jnp.int32, (ROWS, HD), 1) + first
        n = z.shape[1] // HD
        return fold(carry, [z[:, i * HD:(i + 1) * HD] for i in range(n)], [ids + i * HD for i in range(n)], target_col)

    def stats_b(z, first, carry):
        ids = lax.broadcasted_iota(jnp.int32, (8, ROWS), 0) + first
        n = z.shape[0] // 8
        top, acc, hit = carry
        groups = z.reshape(n, 8, ROWS)
        new_top = jnp.maximum(top, jnp.max(groups, axis=0))
        acc = acc * jnp.exp(top - new_top) + jnp.sum(jnp.exp(groups - new_top[None]), axis=0)
        at = lax.broadcasted_iota(jnp.int32, (n, 8, ROWS), 0) * 8 + ids[None]
        hit = hit + jnp.sum(jnp.where(at == target_row[None], groups, 0.0), axis=0)
        return new_top, acc, hit

    def score(ha, hb, size_b):
        sa, sb = head_slot(ha), head_slot(hb)
        za = jnp.zeros((ROWS, CHUNK), F32)
        zb = jnp.zeros((size_b, ROWS), F32)
        for k in range(0, D, DEEP):
            f_k = mbuf[:, k:k + DEEP]
            za = za + mm(f_k, ring[sa, :, k:k + DEEP], NT_DIMS)
            zb = zb + mm(ring[sb, 0:size_b, k:k + DEEP], f_k, NT_DIMS)
        return za, zb

    def refill(h):
        @pl.when(h + SLOTS < NFULL)
        def _():
            head_copy(h + SLOTS).start()

        @pl.when(h + SLOTS == NFULL)
        def _():
            head_copy(NFULL, TAIL).start()

    def empty(shape):
        return jnp.full(shape, -jnp.inf, F32), jnp.zeros(shape, F32), jnp.zeros(shape, F32)

    def pair(i, carry, first):
        h = 2 * i
        head_copy(h).wait()
        head_copy(h + 1).wait()
        now = lax.rem(i, 2)
        za, zb = score(h, h + 1, CHUNK)
        if not first:
            ca, cb = carry
            ca = stats_a(za_buf[1 - now], (h - 2) * CHUNK, ca)
            cb = stats_b(zb_buf[1 - now], (h - 1) * CHUNK, cb)
            carry = (ca, cb)
        za_buf[now] = za
        zb_buf[now] = zb
        refill(h)
        refill(h + 1)
        return carry

    pairs = NFULL // 2
    carry = pair(0, (empty((ROWS, HD)), empty((8, ROWS))), True)
    carry = lax.fori_loop(1, pairs, lambda i, c: pair(i, c, False), carry)
    head_copy(NFULL - 1).wait()
    head_copy(NFULL, TAIL).wait()
    za, zb = score(NFULL - 1, NFULL, TAIL)
    ca, cb = carry
    ca = stats_a(za_buf[(pairs - 1) % 2], (2 * pairs - 2) * CHUNK, ca)
    cb = stats_b(zb_buf[(pairs - 1) % 2], (2 * pairs - 1) * CHUNK, cb)
    ca = stats_a(za, (NFULL - 1) * CHUNK, ca)
    cb = stats_b(zb, NFULL * CHUNK, cb)

    eye = lax.broadcasted_iota(jnp.int32, (ROWS, ROWS), 0) == lax.broadcasted_iota(jnp.int32, (ROWS, ROWS), 1)

    def as_row(col):
        return jnp.sum(jnp.where(eye, jnp.broadcast_to(col, (ROWS, ROWS)), 0.0), axis=0, keepdims=True)

    top_a = jnp.max(ca[0], axis=1, keepdims=True)
    acc_a = as_row(jnp.sum(ca[1] * jnp.exp(ca[0] - top_a), axis=1, keepdims=True))
    hit_a = as_row(jnp.sum(ca[2], axis=1, keepdims=True))
    top_a = as_row(top_a)
    top_b = jnp.max(cb[0], axis=0, keepdims=True)
    acc_b = jnp.sum(cb[1] * jnp.exp(cb[0] - top_b), axis=0, keepdims=True)
    hit_b = jnp.sum(cb[2], axis=0, keepdims=True)
    top = jnp.maximum(top_a, top_b)
    acc = acc_a * jnp.exp(top_a - top) + acc_b * jnp.exp(top_b - top)
    hit = hit_a + hit_b
    st_send[0:1, 0:ROWS] = top
    st_send[1:2, 0:ROWS] = acc
    st_send[2:3, 0:ROWS] = hit
    copies = {}
    for k in order:
        copies[k] = remote(st_send, st_recv.at[k], st_ssem.at[k], st_rsem.at[k], k)
        copies[k].start()
        sends.append(copies[k])
    tops, accs, hits = [top], [acc], [hit]
    for k in reversed(order):
        copies[k].wait_recv()
        tops.append(st_recv[k, 0:1, 0:ROWS])
        accs.append(st_recv[k, 1:2, 0:ROWS])
        hits.append(st_recv[k, 2:3, 0:ROWS])
    best = functools.reduce(jnp.maximum, tops)
    exp_sum = sum(a * jnp.exp(t - best) for t, a in zip(tops, accs))
    lse = best + jnp.log(exp_sum)
    st_ref[0:1, 0:ROWS] = sum(hits) - lse
    st_ref[1:2, 0:ROWS] = lse
    for cp in sends:
        cp.wait_send()
    for cp in y_copies:
        cp.wait()


def finish_kernel(lens_ref, y_hbm, kn_ref, vn_ref, st_ref, kc_hbm, vc_hbm,
                  yo_hbm, ko_hbm, vo_hbm, logp_ref, lse_ref,
                  y_buf, kbuf, vbuf, in_sems, out_sems, y_sems):
    rows = ROWS // PARTS
    y_in = pltpu.make_async_copy(y_hbm, y_buf, y_sems.at[0])
    y_in.start()

    def part(src, dst, sems, i):
        return pltpu.make_async_copy(src.at[pl.ds(i * rows, rows)], dst.at[pl.ds(i * rows, rows)], sems.at[i])

    groups = []
    for i in range(PARTS):
        for idx, (src, buf, dst, new) in enumerate(((kc_hbm, kbuf, ko_hbm, kn_ref), (vc_hbm, vbuf, vo_hbm, vn_ref))):
            copy = part(src, buf, in_sems.at[idx], i)
            copy.start()
            groups.append((i, buf, new, copy, part(buf, dst, out_sems.at[idx], i)))
    logp_ref[...] = st_ref[0, 0:ROWS]
    lse_ref[...] = st_ref[1, 0:ROWS]
    sub = lax.broadcasted_iota(jnp.int32, (16, HD), 0)
    y_in.wait()
    y_out = pltpu.make_async_copy(y_buf, yo_hbm, y_sems.at[1])
    y_out.start()
    for i, buf, new, copy, out in groups:
        copy.wait()
        fresh = new[...].astype(F32)
        for b in range(i * rows, (i + 1) * rows):
            at = lens_ref[b]
            base = pl.multiple_of((at // 16) * 16, 16)
            block = buf[b, pl.ds(base, 16), :].astype(F32)
            row = jnp.broadcast_to(fresh[b:b + 1, :], (16, HD))
            buf[b, pl.ds(base, 16), :] = jnp.where(sub == at - base, row, block).astype(BF16)
        out.start()
    y_out.wait()
    for *_, out in groups:
        out.wait()


def rotary_freqs():
    half = HD // 2
    freq = np.power(THETA, np.arange(half) * (-2.0 / HD)).astype(np.float32)
    return np.concatenate([freq, freq])[None, :]


VM = pl.BlockSpec(memory_space=pltpu.VMEM)
SM = pl.BlockSpec(memory_space=pltpu.SMEM)
HB = pl.BlockSpec(memory_space=pl.ANY)
DMA = pltpu.SemaphoreType.DMA


def local_step(tok_hidden, seq_lens, k_cache, v_cache, next_tok, g_attn, w_q, b_q, w_k, b_k, w_v, b_v, w_o, g_mlp, w_gate, w_up, w_down, g_final, w_head):
    k_cache = k_cache.reshape(ROWS, LMAX, HD)
    v_cache = v_cache.reshape(ROWS, LMAX, HD)
    hidden = jax.ShapeDtypeStruct((ROWS, D), BF16)
    new_row = jax.ShapeDtypeStruct((ROWS, HD), BF16)
    cache = jax.ShapeDtypeStruct((ROWS, LMAX, HD), BF16)
    vector = jax.ShapeDtypeStruct((ROWS,), F32)
    y, k_new, v_new, stats = pl.pallas_call(
        step_kernel,
        out_shape=(hidden, new_row, new_row, jax.ShapeDtypeStruct((8, 128), F32)),
        in_specs=[SM, SM, HB, HB, VM, VM, VM, VM, VM, VM] + [HB] * 10,
        out_specs=(HB, VM, VM, VM),
        scratch_shapes=[
            pltpu.VMEM((SLOTS, CHUNK, D), BF16),
            pltpu.VMEM((ROWS, D), BF16),
            pltpu.VMEM((D,), BF16),
            pltpu.VMEM((D, GROUP * HD), BF16),
            pltpu.VMEM((D, 2 * HD), BF16),
            pltpu.VMEM((ROWS, LMAX, HD), BF16),
            pltpu.VMEM((ROWS, LMAX, HD), BF16),
            pltpu.VMEM((ROWS, GROUP, HD), F32),
            pltpu.VMEM((ROWS, GROUP, LMAX), F32),
            pltpu.VMEM((ROWS, GROUP, HD), F32),
            pltpu.VMEM((ROWS, GROUP * HD), BF16),
            pltpu.VMEM((ROWS, D), BF16),
            pltpu.VMEM((ROWS, FF), F32),
            pltpu.VMEM((ROWS, FF), F32),
            pltpu.VMEM((ROWS, FF), BF16),
            pltpu.VMEM((2, ROWS, CHUNK), F32),
            pltpu.VMEM((2, CHUNK, ROWS), F32),
            pltpu.VMEM((2, NDEV, ROWS, COL), BF16),
            pltpu.VMEM((2, NDEV, ROWS, COL), BF16),
            pltpu.VMEM((2, ROWS, COL), BF16),
            pltpu.VMEM((2, NDEV, ROWS, COL), BF16),
            pltpu.VMEM((8, 128), F32),
            pltpu.VMEM((NDEV, 8, 128), F32),
            DMA((7,)),
            DMA((SLOTS + 8,)),
            DMA((2, NDEV)),
            DMA((2, NDEV)),
            DMA((2, NDEV)),
            DMA((2, NDEV)),
            DMA((NDEV,)),
            DMA((NDEV,)),
            DMA((NDEV,)),
        ],
        compiler_params=pltpu.CompilerParams(collective_id=0, has_side_effects=True, vmem_limit_bytes=VMEM_CAP),
        name='step',
    )(seq_lens, next_tok, tok_hidden, g_attn, g_mlp, g_final, jnp.asarray(rotary_freqs()), b_q, b_k, b_v,
      w_q, w_k, w_v, k_cache, v_cache, w_o, w_gate, w_up, w_down, w_head)
    y_out, k_out, v_out, logp, lse = pl.pallas_call(
        finish_kernel,
        out_shape=(hidden, cache, cache, vector, vector),
        in_specs=[SM, HB, VM, VM, VM, HB, HB],
        out_specs=(HB, HB, HB, VM, VM),
        scratch_shapes=[
            pltpu.VMEM((ROWS, D), BF16),
            pltpu.VMEM((ROWS, LMAX, HD), BF16),
            pltpu.VMEM((ROWS, LMAX, HD), BF16),
            DMA((2, PARTS)),
            DMA((2, PARTS)),
            DMA((2,)),
        ],
        compiler_params=pltpu.CompilerParams(vmem_limit_bytes=VMEM_CAP),
        name='finish',
    )(seq_lens, y, k_new, v_new, stats, k_cache, v_cache)
    shape = (ROWS, LMAX, 1, HD)
    return y_out, k_out.reshape(shape), v_out.reshape(shape), logp, lse


def solution(mesh):
    row_spec = P('dp', None)
    vec_spec = P('dp')
    cache_spec = P('dp', None, 'tp', None)
    col_spec = P(None, 'tp')
    part_spec = P('tp')
    whole_spec = P(None)
    in_specs = (row_spec, vec_spec, cache_spec, cache_spec, vec_spec, whole_spec, col_spec, part_spec, col_spec, part_spec, col_spec, part_spec, P('tp', None), whole_spec, col_spec, col_spec, P('tp', None), whole_spec, P('tp', None))
    out_specs = (row_spec, cache_spec, cache_spec, vec_spec, vec_spec)
    return jax.shard_map(local_step, mesh=mesh, in_specs=in_specs, out_specs=out_specs, check_vma=False)
```

```python
import functools

import jax
import jax.numpy as jnp
import numpy as np
from jax import lax
from jax.experimental import pallas as pl
from jax.experimental.pallas import tpu as pltpu
from jax.sharding import PartitionSpec as P

THETA = 1000000.0
EPS = 1e-6
F32 = jnp.float32
BF16 = jnp.bfloat16
ROWS = 16
D = 4096
HD = 128
GROUP = 4
LMAX = 512
FF = 1792
VOC = 16032
COL = 512
NDEV = 8
SLOTS = 14
CHUNK = 512
DEEP = 256
WO = 3
GU0 = 4
DN0 = 12
HEAD0 = 16
NFULL = VOC // CHUNK
REST = VOC - NFULL * CHUNK
PAIRS = NFULL // 2
QUARTERS = 4
PARTS = 4
VMEM_CAP = 64 * 2**20 - 65536

NT_DIMS = (((1,), (1,)), ((), ()))
NN_DIMS = (((1,), (0,)), ((), ()))


def mm(lhs, rhs, dims=NN_DIMS):
    return lax.dot_general(lhs, rhs, dims, preferred_element_type=F32)


def row_vector(scalars_ref, dtype, shape, axis):
    ids = lax.broadcasted_iota(jnp.int32, shape, axis)
    vec = jnp.zeros(shape, dtype)
    for row in range(ROWS):
        vec = jnp.where(ids == row, scalars_ref[row].astype(dtype), vec)
    return vec


def flip(me, k):
    out = 0
    for bit in (1, 2, 4):
        mine = lax.rem(me // bit, 2)
        out = out + bit * ((1 - mine) if k & bit else mine)
    return out


def norm_cols(parts_ref, gain, out_ref):
    total = jnp.zeros((ROWS, 1), F32)
    for j in range(NDEV):
        part = parts_ref[j].astype(F32)
        total = total + jnp.sum(part * part, axis=-1, keepdims=True)
    inv = lax.rsqrt(total * (1.0 / D) + EPS)
    for j in range(NDEV):
        cols = slice(j * COL, (j + 1) * COL)
        out_ref[:, cols] = (parts_ref[j].astype(F32) * inv * gain[:, cols]).astype(BF16)


def step_kernel(lens_hbm, tok_hbm, x_hbm, ga_hbm, gm_hbm, gf_hbm, freq_hbm, bq_hbm, bk_hbm, bv_hbm,
                wq_hbm, wk_hbm, wv_hbm, kc_hbm, vc_hbm, wo_hbm, wg_hbm, wu_hbm, wd_hbm, wh_hbm,
                y_hbm, kn_hbm, vn_hbm, st_ref,
                ring, lens_ref, tok_ref, x_buf, ga_ref, gm_ref, gf_ref, freq_ref, bq_ref, bk_ref, bv_ref,
                kn_buf, vn_buf, q_scr, s_scr, o_scr, obuf,
                mbuf, gacc, uacc, hbuf, za_buf, zb_buf, rs_send, rs_recv, own, gath, st_send, st_recv,
                small_sems, wq_sems, wkv_sems, cache_sems, ring_sems, last_sems,
                rs_ssem, rs_rsem, ag_ssem, ag_rsem, st_ssem, st_rsem, out_sems):
    me = lax.axis_index('tp')
    peers = {k: flip(me, k) for k in range(1, NDEV)}
    order = (7, 6, 5, 4, 3, 2, 1)
    copy = pltpu.make_async_copy

    def fetch(c):
        slot, sem = ring.at[c % SLOTS], ring_sems.at[c % SLOTS]
        blocks = [pl.ds(j * CHUNK, CHUNK) for j in range(D // CHUNK)]
        if c == 0:
            return [copy(wq_hbm.at[rows, :], slot.at[:, j * COL:(j + 1) * COL], wq_sems.at[j]) for j, rows in enumerate(blocks)]
        if c == 1:
            return [copy(src.at[rows, :], slot.at[:, (2 * j + i) * HD:(2 * j + i + 1) * HD], wkv_sems.at[2 * j + i])
                    for j, rows in enumerate(blocks) for i, src in enumerate((wk_hbm, wv_hbm))]
        if c == 2:
            return [copy(src.at[b], slot.at[:, (i * ROWS + b) * HD:(i * ROWS + b + 1) * HD], cache_sems.at[i * ROWS + b])
                    for i, src in enumerate((kc_hbm, vc_hbm)) for b in range(ROWS)]
        if c == WO:
            return [copy(wo_hbm, slot, sem)]
        if c < DN0:
            rows = pl.ds((c - GU0) * CHUNK, CHUNK)
            return [copy(wg_hbm.at[rows, :], slot.at[:, 0:FF], sem),
                    copy(wu_hbm.at[rows, :], slot.at[:, FF:2 * FF], ring_sems.at[SLOTS + c - GU0])]
        first = (c - DN0) * CHUNK
        size = min(CHUNK, FF - first)
        return [copy(wd_hbm.at[pl.ds(first, size), :], slot.at[0:size, :], sem)]

    def head_slot(h):
        return lax.rem(h + HEAD0, SLOTS)

    def head_row(h):
        return REST + (h - 1) * CHUNK

    def head_rest():
        return copy(wh_hbm.at[0:REST, :], ring.at[HEAD0 % SLOTS, 0:REST, :], ring_sems.at[HEAD0 % SLOTS])

    def head_copy(h):
        slot = head_slot(h)
        return copy(wh_hbm.at[pl.ds(pl.multiple_of(head_row(h), 32), CHUNK), :], ring.at[slot], ring_sems.at[slot])

    def head_quarters(h):
        slot = (h + HEAD0) % SLOTS
        size = D // QUARTERS
        return [copy(wh_hbm.at[pl.ds(head_row(h), CHUNK), q * size:(q + 1) * size], ring.at[slot, :, q * size:(q + 1) * size],
                     last_sems.at[(NFULL - h) * QUARTERS + q]) for q in range(QUARTERS)]

    def start_chunk(c):
        if c < HEAD0:
            for cp in fetch(c):
                cp.start(priority=0 if c < WO else 1)
        elif c == HEAD0:
            head_rest().start(priority=1)
        else:
            head_copy(c - HEAD0).start(priority=1)

    smalls = [copy(src, dst, small_sems.at[i]) for i, (src, dst) in enumerate((
        (x_hbm, x_buf), (ga_hbm, ga_ref), (lens_hbm, lens_ref), (freq_hbm, freq_ref), (bq_hbm, bq_ref), (bk_hbm, bk_ref),
        (bv_hbm, bv_ref), (gm_hbm, gm_ref), (gf_hbm, gf_ref), (tok_hbm, tok_ref)))]
    for cp in smalls:
        cp.start()
    for c in range(SLOTS):
        start_chunk(c)
    barrier = pltpu.get_barrier_semaphore()
    for k in order:
        pl.semaphore_signal(barrier, inc=1, device_id={'tp': peers[k]}, device_id_type=pl.DeviceIdType.MESH)

    for cp in smalls:
        cp.wait()
    angles = row_vector(lens_ref, F32, (ROWS, HD), 0) * freq_ref[...]
    cos = jnp.cos(angles)
    lane = lax.broadcasted_iota(jnp.int32, (ROWS, HD), 1)
    sin = jnp.sin(angles)
    sin = jnp.where(lane < HD // 2, -sin, sin)
    xf = x_buf[...].astype(F32)
    inv = lax.rsqrt(jnp.mean(xf * xf, axis=-1, keepdims=True) + EPS)
    normed = (xf * inv * ga_ref[...].astype(F32)[None, :]).astype(BF16)
    for cp in fetch(0):
        cp.wait()
    q_proj = bq_ref[...].astype(F32)[None, :]
    for j in range(D // CHUNK):
        q_proj = q_proj + mm(normed[:, j * CHUNK:(j + 1) * CHUNK], ring[0, :, j * COL:(j + 1) * COL])
    start_chunk(SLOTS)
    for h in range(GROUP):
        q_h = q_proj[:, h * HD:(h + 1) * HD]
        q_scr[:, h, :] = (q_h * cos + pltpu.roll(q_h, HD // 2, 1) * sin).astype(BF16).astype(F32)
    for cp in fetch(1):
        cp.wait()
    kv_proj = jnp.zeros((ROWS, 2 * HD), F32)
    for j in range(D // CHUNK):
        kv_proj = kv_proj + mm(normed[:, j * CHUNK:(j + 1) * CHUNK], ring[1, :, 2 * j * HD:2 * (j + 1) * HD])
    start_chunk(1 + SLOTS)
    k_proj = kv_proj[:, 0:HD] + bk_ref[...].astype(F32)[None, :]
    k_new = (k_proj * cos + pltpu.roll(k_proj, HD // 2, 1) * sin).astype(BF16)
    v_new = (kv_proj[:, HD:] + bv_ref[...].astype(F32)[None, :]).astype(BF16)
    kn_buf[...] = k_new
    vn_buf[...] = v_new

    for cp in fetch(2):
        cp.wait()
    slot_ids = lax.broadcasted_iota(jnp.int32, (GROUP, LMAX), 1)
    for b in range(ROWS):
        s_b = mm(q_scr[b].astype(BF16), ring[2, :, b * HD:(b + 1) * HD], NT_DIMS) * (HD ** -0.5)
        s_scr[b] = jnp.where(slot_ids < lens_ref[b], s_b, -jnp.inf)
    s_new = jnp.sum(q_scr[...] * k_new.astype(F32)[:, None, :], axis=-1, keepdims=True) * (HD ** -0.5)
    scores = s_scr[...]
    top = jnp.maximum(jnp.max(scores, axis=-1, keepdims=True), s_new)
    e = jnp.exp(scores - top)
    e_new = jnp.exp(s_new - top)
    denom = jnp.sum(e, axis=-1, keepdims=True) + e_new
    s_scr[...] = e / denom
    p_new = (e_new / denom).astype(BF16).astype(F32)
    for b in range(ROWS):
        o_scr[b] = mm(s_scr[b].astype(BF16), ring[2, :, (ROWS + b) * HD:(ROWS + b + 1) * HD])
    o_scr[...] += p_new * v_new.astype(F32)[:, None, :]
    for h in range(GROUP):
        obuf[:, h * HD:(h + 1) * HD] = o_scr[:, h, :].astype(BF16)
    start_chunk(2 + SLOTS)
    outs = [copy(kn_buf, kn_hbm, out_sems.at[NDEV]), copy(vn_buf, vn_hbm, out_sems.at[NDEV + 1])]
    for cp in outs:
        cp.start()

    pl.semaphore_wait(barrier, NDEV - 1)

    def remote(src, dst, ssem, rsem, k):
        return pltpu.make_async_remote_copy(src_ref=src, dst_ref=dst, send_sem=ssem, recv_sem=rsem,
                                            device_id={'tp': peers[k]}, device_id_type=pl.DeviceIdType.MESH)

    sends = []

    def all_reduce(phase, partial, residual, used):
        copies = {}
        for k in order:
            rs_send[phase, k] = partial(peers[k]).astype(BF16)
            copies[k] = remote(rs_send.at[phase, k], rs_recv.at[phase, k], rs_ssem.at[phase, k], rs_rsem.at[phase, k], k)
            copies[k].start()
            sends.append(copies[k])
        total = partial(me)
        for c in used:
            start_chunk(c + SLOTS)
        for k in reversed(order):
            copies[k].wait_recv()
            total = total + rs_recv[phase, k].astype(F32)
        mine = (residual.astype(F32) + total).astype(BF16)
        own[phase] = mine
        gath[phase, me] = mine
        copies = {}
        for k in order:
            copies[k] = remote(own.at[phase], gath.at[phase, me], ag_ssem.at[phase, k], ag_rsem.at[phase, k], k)
            copies[k].start()
            sends.append(copies[k])
        for k in reversed(order):
            copies[k].wait_recv()

    def columns(dev):
        return pl.ds(pl.multiple_of(dev * COL, COL), COL)

    fetch(WO)[0].wait()
    all_reduce(0, lambda dev: mm(obuf[...], ring[WO, :, columns(dev)]), x_buf[:, columns(me)], (WO,))
    norm_cols(gath.at[0], gm_ref[...].astype(F32)[None, :], mbuf)

    for j in range(8):
        for cp in fetch(GU0 + j):
            cp.wait()
        m_j = mbuf[:, j * CHUNK:(j + 1) * CHUNK]
        g_j = mm(m_j, ring[(GU0 + j) % SLOTS, :, 0:FF])
        u_j = mm(m_j, ring[(GU0 + j) % SLOTS, :, FF:2 * FF])
        if j == 0:
            gacc[...] = g_j
            uacc[...] = u_j
        else:
            gacc[...] += g_j
            uacc[...] += u_j
        start_chunk(GU0 + j + SLOTS)
    gate = gacc[...]
    hbuf[...] = (gate * jax.nn.sigmoid(gate) * uacc[...]).astype(BF16)

    for c in range(DN0, HEAD0):
        fetch(c)[0].wait()

    def down(dev):
        total = jnp.zeros((ROWS, COL), F32)
        for j in range(4):
            first, size = j * CHUNK, min(CHUNK, FF - j * CHUNK)
            total = total + mm(hbuf[:, first:first + size], ring[(DN0 + j) % SLOTS, 0:size, columns(dev)])
        return total

    all_reduce(1, down, own[0], range(DN0, HEAD0))
    for j in range(NDEV):
        outs.append(copy(gath.at[1, j], y_hbm.at[:, j * COL:(j + 1) * COL], out_sems.at[j]))
        outs[-1].start()
    norm_cols(gath.at[1], gf_ref[...].astype(F32)[None, :], mbuf)

    target_row = row_vector(tok_ref, jnp.int32, (1, ROWS), 1) - me * VOC
    target_col = row_vector(tok_ref, jnp.int32, (ROWS, 1), 0) - me * VOC

    def fold(carry, pieces, ids, target):
        top, acc, hit = carry
        new_top = functools.reduce(jnp.maximum, pieces, top)
        acc = acc * jnp.exp(top - new_top)
        for piece, at in zip(pieces, ids):
            acc = acc + jnp.exp(piece - new_top)
            hit = hit + jnp.where(at == target, piece, 0.0)
        return new_top, acc, hit

    def stats_a(z, first, carry):
        ids = lax.broadcasted_iota(jnp.int32, (ROWS, HD), 1) + first
        n = z.shape[1] // HD
        return fold(carry, [z[:, i * HD:(i + 1) * HD] for i in range(n)], [ids + i * HD for i in range(n)], target_col)

    def stats_b(z, first, carry):
        ids = lax.broadcasted_iota(jnp.int32, (8, ROWS), 0) + first
        n = z.shape[0] // 8
        top, acc, hit = carry
        groups = z.reshape(n, 8, ROWS)
        new_top = jnp.maximum(top, jnp.max(groups, axis=0))
        acc = acc * jnp.exp(top - new_top) + jnp.sum(jnp.exp(groups - new_top[None]), axis=0)
        at = lax.broadcasted_iota(jnp.int32, (n, 8, ROWS), 0) * 8 + ids[None]
        hit = hit + jnp.sum(jnp.where(at == target_row[None], groups, 0.0), axis=0)
        return new_top, acc, hit

    def score(sa, sb, size_b, first, last, sums):
        sums = list(sums)
        for k in range(first, last, DEEP):
            f_k = mbuf[:, k:k + DEEP]
            for i, q in enumerate(range(0, CHUNK, DEEP)):
                sums[2 * i] = sums[2 * i] + mm(f_k, ring[sa, q:q + DEEP, k:k + DEEP], NT_DIMS)
                if q < size_b:
                    end = min(q + DEEP, size_b)
                    sums[2 * i + 1] = sums[2 * i + 1] + mm(ring[sb, q:end, k:k + DEEP], f_k, NT_DIMS)
        return sums

    def zeros(size_b):
        sums = []
        for q in range(0, CHUNK, DEEP):
            sums += [jnp.zeros((ROWS, DEEP), F32), jnp.zeros((min(DEEP, size_b - q), ROWS), F32) if q < size_b else None]
        return sums

    def empty(shape):
        return jnp.full(shape, -jnp.inf, F32), jnp.zeros(shape, F32), jnp.zeros(shape, F32)

    def keep(sums, now):
        for i, q in enumerate(range(0, CHUNK, DEEP)):
            za_buf[now, :, q:q + DEEP] = sums[2 * i]
            zb_buf[now, q:q + DEEP, :] = sums[2 * i + 1]

    def stats(now, h, carry):
        return stats_a(za_buf[now], head_row(h), carry[0]), stats_b(zb_buf[now], head_row(h + 1), carry[1])

    def refill(h):
        @pl.when(h + SLOTS < 2 * PAIRS)
        def _():
            head_copy(h + SLOTS).start(priority=1)

    head_rest().wait()
    head_copy(1).wait()
    sums = score(head_slot(1), HEAD0 % SLOTS, REST, 0, D, zeros(REST))
    ca = stats_a(sums[0], head_row(1), empty((ROWS, HD)))
    carry = (stats_a(sums[2], head_row(1) + DEEP, ca), stats_b(sums[1], 0, empty((8, ROWS))))
    for h in (0, 1):
        head_copy(h + SLOTS).start(priority=1)

    def pair(i, carry, first=False):
        h = 2 * i
        head_copy(h).wait()
        head_copy(h + 1).wait()
        sums = score(head_slot(h), head_slot(h + 1), CHUNK, 0, D, zeros(CHUNK))
        if not first:
            carry = stats(lax.rem(i - 1, 2), h - 2, carry)
        keep(sums, lax.rem(i, 2))
        refill(h)
        refill(h + 1)

        @pl.when(h + SLOTS == 2 * PAIRS)
        def _():
            for q in range(QUARTERS):
                for cp in (last_a[q], last_b[q]):
                    cp.start(priority=1)
        return carry

    last_a, last_b = head_quarters(2 * PAIRS), head_quarters(2 * PAIRS + 1)
    carry = pair(1, carry, True)
    carry = lax.fori_loop(2, PAIRS, pair, carry)
    sums = zeros(CHUNK)
    size = D // QUARTERS
    for q in range(QUARTERS):
        last_a[q].wait()
        last_b[q].wait()
        sums = score((2 * PAIRS + HEAD0) % SLOTS, (2 * PAIRS + 1 + HEAD0) % SLOTS, CHUNK, q * size, (q + 1) * size, sums)
        if q == 0:
            carry = stats((PAIRS - 1) % 2, 2 * PAIRS - 2, carry)
    ca, cb = carry
    for i, q in enumerate(range(0, CHUNK, DEEP)):
        ca = stats_a(sums[2 * i], head_row(2 * PAIRS) + q, ca)
        cb = stats_b(sums[2 * i + 1], head_row(2 * PAIRS + 1) + q, cb)

    eye = lax.broadcasted_iota(jnp.int32, (ROWS, ROWS), 0) == lax.broadcasted_iota(jnp.int32, (ROWS, ROWS), 1)

    def as_row(col):
        return jnp.sum(jnp.where(eye, jnp.broadcast_to(col, (ROWS, ROWS)), 0.0), axis=0, keepdims=True)

    top_a = jnp.max(ca[0], axis=1, keepdims=True)
    acc_a = as_row(jnp.sum(ca[1] * jnp.exp(ca[0] - top_a), axis=1, keepdims=True))
    hit_a = as_row(jnp.sum(ca[2], axis=1, keepdims=True))
    top_a = as_row(top_a)
    top_b = jnp.max(cb[0], axis=0, keepdims=True)
    acc_b = jnp.sum(cb[1] * jnp.exp(cb[0] - top_b), axis=0, keepdims=True)
    hit_b = jnp.sum(cb[2], axis=0, keepdims=True)
    top = jnp.maximum(top_a, top_b)
    acc = acc_a * jnp.exp(top_a - top) + acc_b * jnp.exp(top_b - top)
    hit = hit_a + hit_b
    st_send[0:1, 0:ROWS] = top
    st_send[1:2, 0:ROWS] = acc
    st_send[2:3, 0:ROWS] = hit
    copies = {}
    for k in order:
        copies[k] = remote(st_send, st_recv.at[k], st_ssem.at[k], st_rsem.at[k], k)
        copies[k].start()
        sends.append(copies[k])
    tops, accs, hits = [top], [acc], [hit]
    for k in reversed(order):
        copies[k].wait_recv()
        tops.append(st_recv[k, 0:1, 0:ROWS])
        accs.append(st_recv[k, 1:2, 0:ROWS])
        hits.append(st_recv[k, 2:3, 0:ROWS])
    best = functools.reduce(jnp.maximum, tops)
    exp_sum = sum(a * jnp.exp(t - best) for t, a in zip(tops, accs))
    lse = best + jnp.log(exp_sum)
    st_ref[0:1, 0:ROWS] = sum(hits) - lse
    st_ref[1:2, 0:ROWS] = lse
    for cp in sends:
        cp.wait_send()
    for cp in outs:
        cp.wait()


def finish_kernel(lens_hbm, y_hbm, kn_hbm, vn_hbm, st_hbm, kc_hbm, vc_hbm,
                  yo_hbm, ko_hbm, vo_hbm, logp_hbm, lse_hbm,
                  lens_ref, y_buf, kn_ref, vn_ref, st_ref, logp_ref, lse_ref, kbuf, vbuf, in_sems, out_sems, small_sems):
    rows = ROWS // PARTS
    copy = pltpu.make_async_copy

    def part(src, dst, sems, i):
        return copy(src.at[pl.ds(i * rows, rows)], dst.at[pl.ds(i * rows, rows)], sems.at[i])

    smalls = [copy(src, dst, small_sems.at[i]) for i, (src, dst) in enumerate((
        (lens_hbm, lens_ref), (kn_hbm, kn_ref), (vn_hbm, vn_ref), (st_hbm, st_ref), (y_hbm, y_buf)))]
    for cp in smalls:
        cp.start()
    groups = []
    for i in range(PARTS):
        for idx, (src, buf, dst, new) in enumerate(((kc_hbm, kbuf, ko_hbm, kn_ref), (vc_hbm, vbuf, vo_hbm, vn_ref))):
            fill = part(src, buf, in_sems.at[idx], i)
            fill.start()
            groups.append((i, buf, new, fill, part(buf, dst, out_sems.at[idx], i)))
    sub = lax.broadcasted_iota(jnp.int32, (16, HD), 0)
    for cp in smalls:
        cp.wait()
    logp_ref[...] = st_ref[0, 0:ROWS]
    lse_ref[...] = st_ref[1, 0:ROWS]
    outs = [copy(y_buf, yo_hbm, small_sems.at[5]), copy(logp_ref, logp_hbm, small_sems.at[6]), copy(lse_ref, lse_hbm, small_sems.at[7])]
    for i, buf, new, fill, out in groups:
        fill.wait()
        fresh = new[...].astype(F32)
        for b in range(i * rows, (i + 1) * rows):
            at = lens_ref[b]
            base = pl.multiple_of((at // 16) * 16, 16)
            block = buf[b, pl.ds(base, 16), :].astype(F32)
            row = jnp.broadcast_to(fresh[b:b + 1, :], (16, HD))
            buf[b, pl.ds(base, 16), :] = jnp.where(sub == at - base, row, block).astype(BF16)
        out.start()
        if outs and i == 0:
            for cp in outs:
                cp.start()
            waits, outs = outs, []
    for cp in waits:
        cp.wait()
    for *_, out in groups:
        out.wait()


def rotary_freqs():
    half = HD // 2
    freq = np.power(THETA, np.arange(half) * (-2.0 / HD)).astype(np.float32)
    return np.concatenate([freq, freq])[None, :]


VM = pl.BlockSpec(memory_space=pltpu.VMEM)
HB = pl.BlockSpec(memory_space=pl.ANY)
DMA = pltpu.SemaphoreType.DMA


def local_step(tok_hidden, seq_lens, k_cache, v_cache, next_tok, g_attn, w_q, b_q, w_k, b_k, w_v, b_v, w_o, g_mlp, w_gate, w_up, w_down, g_final, w_head):
    k_cache = k_cache.reshape(ROWS, LMAX, HD)
    v_cache = v_cache.reshape(ROWS, LMAX, HD)
    hidden = jax.ShapeDtypeStruct((ROWS, D), BF16)
    new_row = jax.ShapeDtypeStruct((ROWS, HD), BF16)
    cache = jax.ShapeDtypeStruct((ROWS, LMAX, HD), BF16)
    vector = jax.ShapeDtypeStruct((ROWS,), F32)
    y, k_new, v_new, stats = pl.pallas_call(
        step_kernel,
        out_shape=(hidden, new_row, new_row, jax.ShapeDtypeStruct((8, 128), F32)),
        in_specs=[HB] * 20,
        out_specs=(HB, HB, HB, VM),
        scratch_shapes=[
            pltpu.VMEM((SLOTS, CHUNK, D), BF16),
            pltpu.SMEM((ROWS,), jnp.int32),
            pltpu.SMEM((ROWS,), jnp.int32),
            pltpu.VMEM((ROWS, D), BF16),
            pltpu.VMEM((D,), BF16),
            pltpu.VMEM((D,), BF16),
            pltpu.VMEM((D,), BF16),
            pltpu.VMEM((1, HD), F32),
            pltpu.VMEM((GROUP * HD,), BF16),
            pltpu.VMEM((HD,), BF16),
            pltpu.VMEM((HD,), BF16),
            pltpu.VMEM((ROWS, HD), BF16),
            pltpu.VMEM((ROWS, HD), BF16),
            pltpu.VMEM((ROWS, GROUP, HD), F32),
            pltpu.VMEM((ROWS, GROUP, LMAX), F32),
            pltpu.VMEM((ROWS, GROUP, HD), F32),
            pltpu.VMEM((ROWS, GROUP * HD), BF16),
            pltpu.VMEM((ROWS, D), BF16),
            pltpu.VMEM((ROWS, FF), F32),
            pltpu.VMEM((ROWS, FF), F32),
            pltpu.VMEM((ROWS, FF), BF16),
            pltpu.VMEM((2, ROWS, CHUNK), F32),
            pltpu.VMEM((2, CHUNK, ROWS), F32),
            pltpu.VMEM((2, NDEV, ROWS, COL), BF16),
            pltpu.VMEM((2, NDEV, ROWS, COL), BF16),
            pltpu.VMEM((2, ROWS, COL), BF16),
            pltpu.VMEM((2, NDEV, ROWS, COL), BF16),
            pltpu.VMEM((8, 128), F32),
            pltpu.VMEM((NDEV, 8, 128), F32),
            DMA((10,)),
            DMA((8,)),
            DMA((16,)),
            DMA((2 * ROWS,)),
            DMA((SLOTS + 8,)),
            DMA((2 * QUARTERS,)),
            DMA((2, NDEV)),
            DMA((2, NDEV)),
            DMA((2, NDEV)),
            DMA((2, NDEV)),
            DMA((NDEV,)),
            DMA((NDEV,)),
            DMA((NDEV + 2,)),
        ],
        compiler_params=pltpu.CompilerParams(collective_id=0, has_side_effects=True, vmem_limit_bytes=VMEM_CAP),
        name='step',
    )(seq_lens, next_tok, tok_hidden, g_attn, g_mlp, g_final, jnp.asarray(rotary_freqs()), b_q, b_k, b_v,
      w_q, w_k, w_v, k_cache, v_cache, w_o, w_gate, w_up, w_down, w_head)
    y_out, k_out, v_out, logp, lse = pl.pallas_call(
        finish_kernel,
        out_shape=(hidden, cache, cache, vector, vector),
        in_specs=[HB] * 7,
        out_specs=(HB,) * 5,
        scratch_shapes=[
            pltpu.SMEM((ROWS,), jnp.int32),
            pltpu.VMEM((ROWS, D), BF16),
            pltpu.VMEM((ROWS, HD), BF16),
            pltpu.VMEM((ROWS, HD), BF16),
            pltpu.VMEM((8, 128), F32),
            pltpu.VMEM((ROWS,), F32),
            pltpu.VMEM((ROWS,), F32),
            pltpu.VMEM((ROWS, LMAX, HD), BF16),
            pltpu.VMEM((ROWS, LMAX, HD), BF16),
            DMA((2, PARTS)),
            DMA((2, PARTS)),
            DMA((8,)),
        ],
        compiler_params=pltpu.CompilerParams(vmem_limit_bytes=VMEM_CAP),
        name='finish',
    )(seq_lens, y, k_new, v_new, stats, k_cache, v_cache)
    shape = (ROWS, LMAX, 1, HD)
    return y_out, k_out.reshape(shape), v_out.reshape(shape), logp, lse


def solution(mesh):
    row_spec = P('dp', None)
    vec_spec = P('dp')
    cache_spec = P('dp', None, 'tp', None)
    col_spec = P(None, 'tp')
    part_spec = P('tp')
    whole_spec = P(None)
    in_specs = (row_spec, vec_spec, cache_spec, cache_spec, vec_spec, whole_spec, col_spec, part_spec, col_spec, part_spec, col_spec, part_spec, P('tp', None), whole_spec, col_spec, col_spec, P('tp', None), whole_spec, P('tp', None))
    out_specs = (row_spec, cache_spec, cache_spec, vec_spec, vec_spec)
    return jax.shard_map(local_step, mesh=mesh, in_specs=in_specs, out_specs=out_specs, check_vma=False)
```

```python
import functools

import jax
import jax.numpy as jnp
import numpy as np
from jax import lax
from jax.experimental import pallas as pl
from jax.experimental.pallas import tpu as pltpu
from jax.sharding import PartitionSpec as P

THETA = 1000000.0
EPS = 1e-6
F32 = jnp.float32
BF16 = jnp.bfloat16
ROWS = 16
D = 4096
HD = 128
GROUP = 4
LMAX = 512
FF = 1792
VOC = 16032
COL = 512
NDEV = 8
SLOTS = 12
CHUNK = 512
DEEP = 256
WO = 2
GU0 = 3
DN0 = 11
HEAD0 = 15
NFULL = VOC // CHUNK
REST = VOC - NFULL * CHUNK
PAIRS = NFULL // 2
QUARTERS = 4
STEP_VMEM = 56 * 2**20

NT_DIMS = (((1,), (1,)), ((), ()))
NN_DIMS = (((1,), (0,)), ((), ()))


def mm(lhs, rhs, dims=NN_DIMS):
    return lax.dot_general(lhs, rhs, dims, preferred_element_type=F32)


def row_vector(scalars_ref, dtype, shape, axis):
    ids = lax.broadcasted_iota(jnp.int32, shape, axis)
    vec = jnp.zeros(shape, dtype)
    for row in range(ROWS):
        vec = jnp.where(ids == row, scalars_ref[row].astype(dtype), vec)
    return vec


def flip(me, k):
    out = 0
    for bit in (1, 2, 4):
        mine = lax.rem(me // bit, 2)
        out = out + bit * ((1 - mine) if k & bit else mine)
    return out


def norm_cols(parts_ref, gain, out_ref):
    total = jnp.zeros((ROWS, 1), F32)
    for j in range(NDEV):
        part = parts_ref[j].astype(F32)
        total = total + jnp.sum(part * part, axis=-1, keepdims=True)
    inv = lax.rsqrt(total * (1.0 / D) + EPS)
    for j in range(NDEV):
        cols = slice(j * COL, (j + 1) * COL)
        out_ref[:, cols] = (parts_ref[j].astype(F32) * inv * gain[:, cols]).astype(BF16)


def step_kernel(lens_hbm, tok_hbm, x_hbm, ga_hbm, gm_hbm, gf_hbm, freq_hbm, bq_hbm, bk_hbm, bv_hbm,
                wq_hbm, wk_hbm, wv_hbm, kc_hbm, vc_hbm, wo_hbm, wg_hbm, wu_hbm, wd_hbm, wh_hbm,
                y_ref, k_ref, v_ref, st_ref,
                ring, lens_ref, tok_ref, x_buf, ga_ref, gm_ref, gf_ref, freq_ref, bq_ref, bk_ref, bv_ref,
                q_scr, s_scr, o_scr, obuf,
                mbuf, gacc, uacc, hbuf, za_buf, zb_buf, rs_send, rs_recv, own, gath, st_send, st_recv,
                small_sems, cache_sems, ring_sems, last_sems, send_sems, recv_sems):
    me = lax.axis_index('tp')
    peers = {k: flip(me, k) for k in range(1, NDEV)}
    order = (7, 6, 5, 4, 3, 2, 1)
    copy = pltpu.make_async_copy

    def fetch(c):
        slot, sem = ring.at[c % SLOTS], ring_sems.at[c % SLOTS]
        blocks = [pl.ds(j * CHUNK, CHUNK) for j in range(D // CHUNK)]
        if c == 0:
            return [copy(wq_hbm.at[rows, :], slot.at[:, j * COL:(j + 1) * COL], sem) for j, rows in enumerate(blocks)]
        if c == 1:
            return [copy(src.at[rows, :], slot.at[:, (2 * j + i) * HD:(2 * j + i + 1) * HD], sem)
                    for j, rows in enumerate(blocks) for i, src in enumerate((wk_hbm, wv_hbm))]
        if c == WO:
            return [copy(wo_hbm, slot, sem)]
        if c < DN0:
            rows = pl.ds((c - GU0) * CHUNK, CHUNK)
            return [copy(wg_hbm.at[rows, :], slot.at[:, 0:FF], sem),
                    copy(wu_hbm.at[rows, :], slot.at[:, FF:2 * FF], sem)]
        first = (c - DN0) * CHUNK
        size = min(CHUNK, FF - first)
        return [copy(wd_hbm.at[pl.ds(first, size), :], slot.at[0:size, :], sem)]

    def landed(c):
        width = {0: D, 1: 2 * HD * (D // CHUNK)}.get(c, 2 * FF if GU0 <= c < DN0 else D)
        rows = min(CHUNK, FF - (c - DN0) * CHUNK) if c >= DN0 else CHUNK
        copy(wo_hbm.at[0:rows, 0:width], ring.at[c % SLOTS, 0:rows, 0:width], ring_sems.at[c % SLOTS]).wait()

    def head_slot(h):
        return lax.rem(h + HEAD0, SLOTS)

    def head_row(h):
        return REST + (h - 1) * CHUNK

    def head_rest():
        return copy(wh_hbm.at[0:REST, :], ring.at[HEAD0 % SLOTS, 0:REST, :], ring_sems.at[HEAD0 % SLOTS])

    def head_copy(h):
        slot = head_slot(h)
        return copy(wh_hbm.at[pl.ds(pl.multiple_of(head_row(h), 32), CHUNK), :], ring.at[slot], ring_sems.at[slot])

    def head_quarters(h):
        slot = (h + HEAD0) % SLOTS
        size = D // QUARTERS
        return [copy(wh_hbm.at[pl.ds(head_row(h), CHUNK), q * size:(q + 1) * size], ring.at[slot, :, q * size:(q + 1) * size],
                     last_sems.at[q]) for q in range(QUARTERS)]

    def start_chunk(c):
        if c < HEAD0:
            for cp in fetch(c):
                cp.start(priority=0 if c < WO else 1)
        elif c == HEAD0:
            head_rest().start(priority=1)
        else:
            head_copy(c - HEAD0).start(priority=1)

    smalls = [copy(src, dst, small_sems.at[i]) for i, (src, dst) in enumerate((
        (x_hbm, x_buf), (ga_hbm, ga_ref), (lens_hbm, lens_ref), (freq_hbm, freq_ref), (bq_hbm, bq_ref), (bk_hbm, bk_ref),
        (bv_hbm, bv_ref), (gm_hbm, gm_ref), (gf_hbm, gf_ref), (tok_hbm, tok_ref)))]
    for cp in smalls:
        cp.start()
    caches = [copy(kc_hbm, k_ref, cache_sems.at[0]), copy(vc_hbm, v_ref, cache_sems.at[1])]
    for c in range(SLOTS):
        if c == WO:
            for cp in caches:
                cp.start()
        start_chunk(c)
    barrier = pltpu.get_barrier_semaphore()
    for k in order:
        pl.semaphore_signal(barrier, inc=1, device_id={'tp': peers[k]}, device_id_type=pl.DeviceIdType.MESH)

    for cp in smalls:
        cp.wait()
    angles = row_vector(lens_ref, F32, (ROWS, HD), 0) * freq_ref[...]
    cos = jnp.cos(angles)
    lane = lax.broadcasted_iota(jnp.int32, (ROWS, HD), 1)
    sin = jnp.sin(angles)
    sin = jnp.where(lane < HD // 2, -sin, sin)
    xf = x_buf[...].astype(F32)
    inv = lax.rsqrt(jnp.mean(xf * xf, axis=-1, keepdims=True) + EPS)
    normed = (xf * inv * ga_ref[...].astype(F32)[None, :]).astype(BF16)
    landed(0)
    q_proj = bq_ref[...].astype(F32)[None, :]
    for j in range(D // CHUNK):
        q_proj = q_proj + mm(normed[:, j * CHUNK:(j + 1) * CHUNK], ring[0, :, j * COL:(j + 1) * COL])
    start_chunk(SLOTS)
    for h in range(GROUP):
        q_h = q_proj[:, h * HD:(h + 1) * HD]
        q_scr[:, h, :] = (q_h * cos + pltpu.roll(q_h, HD // 2, 1) * sin).astype(BF16).astype(F32)
    landed(1)
    kv_proj = jnp.zeros((ROWS, 2 * HD), F32)
    for j in range(D // CHUNK):
        kv_proj = kv_proj + mm(normed[:, j * CHUNK:(j + 1) * CHUNK], ring[1, :, 2 * j * HD:2 * (j + 1) * HD])
    start_chunk(1 + SLOTS)
    k_proj = kv_proj[:, 0:HD] + bk_ref[...].astype(F32)[None, :]
    k_new = (k_proj * cos + pltpu.roll(k_proj, HD // 2, 1) * sin).astype(BF16)
    v_new = (kv_proj[:, HD:] + bv_ref[...].astype(F32)[None, :]).astype(BF16)

    caches[0].wait()
    slot_ids = lax.broadcasted_iota(jnp.int32, (GROUP, LMAX), 1)
    for b in range(ROWS):
        s_b = mm(q_scr[b].astype(BF16), k_ref[b], NT_DIMS) * (HD ** -0.5)
        s_scr[b] = jnp.where(slot_ids < lens_ref[b], s_b, -jnp.inf)
    s_new = jnp.sum(q_scr[...] * k_new.astype(F32)[:, None, :], axis=-1, keepdims=True) * (HD ** -0.5)
    scores = s_scr[...]
    top = jnp.maximum(jnp.max(scores, axis=-1, keepdims=True), s_new)
    e = jnp.exp(scores - top)
    e_new = jnp.exp(s_new - top)
    denom = jnp.sum(e, axis=-1, keepdims=True) + e_new
    s_scr[...] = e / denom
    p_new = (e_new / denom).astype(BF16).astype(F32)
    caches[1].wait()
    for b in range(ROWS):
        o_scr[b] = mm(s_scr[b].astype(BF16), v_ref[b])
    o_scr[...] += p_new * v_new.astype(F32)[:, None, :]
    for h in range(GROUP):
        obuf[:, h * HD:(h + 1) * HD] = o_scr[:, h, :].astype(BF16)

    pl.semaphore_wait(barrier, NDEV - 1)

    def remote(src, dst, ssem, rsem, k):
        return pltpu.make_async_remote_copy(src_ref=src, dst_ref=dst, send_sem=ssem, recv_sem=rsem,
                                            device_id={'tp': peers[k]}, device_id_type=pl.DeviceIdType.MESH)

    def exchange(phase, payload, landing, size):
        for k in order:
            remote(payload(k), landing(k), send_sems.at[phase], recv_sems.at[phase], k).start()
        return remote(size, size, send_sems.at[phase], recv_sems.at[phase], 1)

    def all_reduce(phase, partial, residual, used, meanwhile):
        def send_part(k):
            rs_send[phase, k] = partial(peers[k]).astype(BF16)
            return rs_send.at[phase, k]

        seven = rs_recv.at[phase, 1:NDEV]
        scatter = exchange(2 * phase, send_part, lambda k: rs_recv.at[phase, k], seven)
        total = partial(me)
        for c in used:
            start_chunk(c + SLOTS)
        meanwhile()
        scatter.wait_recv()
        for k in reversed(order):
            total = total + rs_recv[phase, k].astype(F32)
        mine = (residual.astype(F32) + total).astype(BF16)
        own[phase] = mine
        gath[phase, me] = mine
        gather = exchange(2 * phase + 1, lambda k: own.at[phase], lambda k: gath.at[phase, me], seven)
        gather.wait_recv()
        return [scatter, gather]

    def columns(dev):
        return pl.ds(pl.multiple_of(dev * COL, COL), COL)

    def insert():
        ids = lax.broadcasted_iota(jnp.int32, (LMAX, HD), 0)
        for b in range(ROWS):
            here = ids == lens_ref[b]
            for ref, new in ((k_ref, k_new), (v_ref, v_new)):
                row = jnp.broadcast_to(new[b:b + 1, :].astype(F32), (LMAX, HD))
                ref[b] = jnp.where(here, row, ref[b].astype(F32)).astype(BF16)

    landed(WO)
    sends = all_reduce(0, lambda dev: mm(obuf[...], ring[WO, :, columns(dev)]), x_buf[:, columns(me)], (WO,), insert)
    norm_cols(gath.at[0], gm_ref[...].astype(F32)[None, :], mbuf)

    for j in range(8):
        landed(GU0 + j)
        m_j = mbuf[:, j * CHUNK:(j + 1) * CHUNK]
        g_j = mm(m_j, ring[(GU0 + j) % SLOTS, :, 0:FF])
        u_j = mm(m_j, ring[(GU0 + j) % SLOTS, :, FF:2 * FF])
        if j == 0:
            gacc[...] = g_j
            uacc[...] = u_j
        else:
            gacc[...] += g_j
            uacc[...] += u_j
        start_chunk(GU0 + j + SLOTS)
    gate = gacc[...]
    hbuf[...] = (gate * jax.nn.sigmoid(gate) * uacc[...]).astype(BF16)

    for c in range(DN0, HEAD0):
        landed(c)

    def down(dev):
        total = jnp.zeros((ROWS, COL), F32)
        for j in range(4):
            first, size = j * CHUNK, min(CHUNK, FF - j * CHUNK)
            total = total + mm(hbuf[:, first:first + size], ring[(DN0 + j) % SLOTS, 0:size, columns(dev)])
        return total

    sends += all_reduce(1, down, own[0], range(DN0, HEAD0), lambda: None)
    for j in range(NDEV):
        y_ref[:, j * COL:(j + 1) * COL] = gath[1, j]
    norm_cols(gath.at[1], gf_ref[...].astype(F32)[None, :], mbuf)

    target_row = row_vector(tok_ref, jnp.int32, (1, ROWS), 1) - me * VOC
    target_col = row_vector(tok_ref, jnp.int32, (ROWS, 1), 0) - me * VOC

    def fold(carry, pieces, ids, target):
        top, acc, hit = carry
        new_top = functools.reduce(jnp.maximum, pieces, top)
        acc = acc * jnp.exp(top - new_top)
        for piece, at in zip(pieces, ids):
            acc = acc + jnp.exp(piece - new_top)
            hit = hit + jnp.where(at == target, piece, 0.0)
        return new_top, acc, hit

    def stats_a(z, first, carry):
        ids = lax.broadcasted_iota(jnp.int32, (ROWS, HD), 1) + first
        n = z.shape[1] // HD
        return fold(carry, [z[:, i * HD:(i + 1) * HD] for i in range(n)], [ids + i * HD for i in range(n)], target_col)

    def stats_b(z, first, carry):
        ids = lax.broadcasted_iota(jnp.int32, (8, ROWS), 0) + first
        n = z.shape[0] // 8
        top, acc, hit = carry
        groups = z.reshape(n, 8, ROWS)
        new_top = jnp.maximum(top, jnp.max(groups, axis=0))
        acc = acc * jnp.exp(top - new_top) + jnp.sum(jnp.exp(groups - new_top[None]), axis=0)
        at = lax.broadcasted_iota(jnp.int32, (n, 8, ROWS), 0) * 8 + ids[None]
        hit = hit + jnp.sum(jnp.where(at == target_row[None], groups, 0.0), axis=0)
        return new_top, acc, hit

    def score(sa, sb, size_b, first, last, sums):
        sums = list(sums)
        for k in range(first, last, DEEP):
            f_k = mbuf[:, k:k + DEEP]
            for i, q in enumerate(range(0, CHUNK, DEEP)):
                sums[2 * i] = sums[2 * i] + mm(f_k, ring[sa, q:q + DEEP, k:k + DEEP], NT_DIMS)
                if q < size_b:
                    end = min(q + DEEP, size_b)
                    sums[2 * i + 1] = sums[2 * i + 1] + mm(ring[sb, q:end, k:k + DEEP], f_k, NT_DIMS)
        return sums

    def zeros(size_b):
        sums = []
        for q in range(0, CHUNK, DEEP):
            sums += [jnp.zeros((ROWS, DEEP), F32), jnp.zeros((min(DEEP, size_b - q), ROWS), F32) if q < size_b else None]
        return sums

    def empty(shape):
        return jnp.full(shape, -jnp.inf, F32), jnp.zeros(shape, F32), jnp.zeros(shape, F32)

    def keep(sums, now):
        for i, q in enumerate(range(0, CHUNK, DEEP)):
            za_buf[now, :, q:q + DEEP] = sums[2 * i]
            zb_buf[now, q:q + DEEP, :] = sums[2 * i + 1]

    def stats(now, h, carry):
        return stats_a(za_buf[now], head_row(h), carry[0]), stats_b(zb_buf[now], head_row(h + 1), carry[1])

    def refill(h):
        @pl.when(h + SLOTS < 2 * PAIRS)
        def _():
            head_copy(h + SLOTS).start(priority=1)

    head_rest().wait()
    head_copy(1).wait()
    sums = score(head_slot(1), HEAD0 % SLOTS, REST, 0, D, zeros(REST))
    ca = stats_a(sums[0], head_row(1), empty((ROWS, HD)))
    carry = (stats_a(sums[2], head_row(1) + DEEP, ca), stats_b(sums[1], 0, empty((8, ROWS))))
    for h in (0, 1):
        head_copy(h + SLOTS).start(priority=1)

    def pair(i, carry, first=False):
        h = 2 * i
        head_copy(h).wait()
        head_copy(h + 1).wait()
        sums = score(head_slot(h), head_slot(h + 1), CHUNK, 0, D, zeros(CHUNK))
        if not first:
            carry = stats(lax.rem(i - 1, 2), h - 2, carry)
        keep(sums, lax.rem(i, 2))
        refill(h)
        refill(h + 1)

        @pl.when(h + SLOTS == 2 * PAIRS)
        def _():
            for q in range(QUARTERS):
                for cp in (last_a[q], last_b[q]):
                    cp.start(priority=1)
        return carry

    last_a, last_b = head_quarters(2 * PAIRS), head_quarters(2 * PAIRS + 1)
    carry = pair(1, carry, True)
    carry = lax.fori_loop(2, PAIRS, pair, carry)
    sums = zeros(CHUNK)
    size = D // QUARTERS
    for q in range(QUARTERS):
        copy(wo_hbm.at[:, 0:2 * size], ring.at[0, :, 0:2 * size], last_sems.at[q]).wait()
        sums = score((2 * PAIRS + HEAD0) % SLOTS, (2 * PAIRS + 1 + HEAD0) % SLOTS, CHUNK, q * size, (q + 1) * size, sums)
        if q == 0:
            carry = stats((PAIRS - 1) % 2, 2 * PAIRS - 2, carry)
    ca, cb = carry
    for i, q in enumerate(range(0, CHUNK, DEEP)):
        ca = stats_a(sums[2 * i], head_row(2 * PAIRS) + q, ca)
        cb = stats_b(sums[2 * i + 1], head_row(2 * PAIRS + 1) + q, cb)

    eye = lax.broadcasted_iota(jnp.int32, (ROWS, ROWS), 0) == lax.broadcasted_iota(jnp.int32, (ROWS, ROWS), 1)

    def as_row(col):
        return jnp.sum(jnp.where(eye, jnp.broadcast_to(col, (ROWS, ROWS)), 0.0), axis=0, keepdims=True)

    top_a = jnp.max(ca[0], axis=1, keepdims=True)
    acc_a = as_row(jnp.sum(ca[1] * jnp.exp(ca[0] - top_a), axis=1, keepdims=True))
    hit_a = as_row(jnp.sum(ca[2], axis=1, keepdims=True))
    top_a = as_row(top_a)
    top_b = jnp.max(cb[0], axis=0, keepdims=True)
    acc_b = jnp.sum(cb[1] * jnp.exp(cb[0] - top_b), axis=0, keepdims=True)
    hit_b = jnp.sum(cb[2], axis=0, keepdims=True)
    top = jnp.maximum(top_a, top_b)
    acc = acc_a * jnp.exp(top_a - top) + acc_b * jnp.exp(top_b - top)
    hit = hit_a + hit_b
    st_send[0:1, 0:ROWS] = top
    st_send[1:2, 0:ROWS] = acc
    st_send[2:3, 0:ROWS] = hit
    share = exchange(4, lambda k: st_send, lambda k: st_recv.at[k], st_recv.at[1:NDEV])
    share.wait_recv()
    tops, accs, hits = [top], [acc], [hit]
    for k in reversed(order):
        tops.append(st_recv[k, 0:1, 0:ROWS])
        accs.append(st_recv[k, 1:2, 0:ROWS])
        hits.append(st_recv[k, 2:3, 0:ROWS])
    best = functools.reduce(jnp.maximum, tops)
    exp_sum = sum(a * jnp.exp(t - best) for t, a in zip(tops, accs))
    lse = best + jnp.log(exp_sum)
    st_ref[0:1, 0:ROWS] = sum(hits) - lse
    st_ref[1:2, 0:ROWS] = lse
    for group in sends + [share]:
        group.wait_send()


def finish_kernel(y_ref, k_ref, v_ref, st_ref, y_hbm, k_hbm, v_hbm, logp_hbm, lse_hbm, logp_ref, lse_ref, sems):
    logp_ref[...] = st_ref[0, 0:ROWS]
    lse_ref[...] = st_ref[1, 0:ROWS]
    copies = [pltpu.make_async_copy(src, dst, sems.at[i]) for i, (src, dst) in enumerate((
        (k_ref, k_hbm), (v_ref, v_hbm), (y_ref, y_hbm), (logp_ref, logp_hbm), (lse_ref, lse_hbm)))]
    for cp in copies:
        cp.start()
    for cp in copies:
        cp.wait()


def rotary_freqs():
    half = HD // 2
    freq = np.power(THETA, np.arange(half) * (-2.0 / HD)).astype(np.float32)
    return np.concatenate([freq, freq])[None, :]


VM = pl.BlockSpec(memory_space=pltpu.VMEM)
HB = pl.BlockSpec(memory_space=pl.ANY)
DMA = pltpu.SemaphoreType.DMA


def local_step(tok_hidden, seq_lens, k_cache, v_cache, next_tok, g_attn, w_q, b_q, w_k, b_k, w_v, b_v, w_o, g_mlp, w_gate, w_up, w_down, g_final, w_head):
    k_cache = k_cache.reshape(ROWS, LMAX, HD)
    v_cache = v_cache.reshape(ROWS, LMAX, HD)
    hidden = jax.ShapeDtypeStruct((ROWS, D), BF16)
    cache = jax.ShapeDtypeStruct((ROWS, LMAX, HD), BF16)
    vector = jax.ShapeDtypeStruct((ROWS,), F32)
    y, k_all, v_all, stats = pl.pallas_call(
        step_kernel,
        out_shape=(pltpu.VMEM((ROWS, D), BF16), pltpu.VMEM((ROWS, LMAX, HD), BF16), pltpu.VMEM((ROWS, LMAX, HD), BF16),
                   pltpu.VMEM((8, 128), F32)),
        in_specs=[HB] * 20,
        out_specs=(VM,) * 4,
        scratch_shapes=[
            pltpu.VMEM((SLOTS, CHUNK, D), BF16),
            pltpu.SMEM((ROWS,), jnp.int32),
            pltpu.SMEM((ROWS,), jnp.int32),
            pltpu.VMEM((ROWS, D), BF16),
            pltpu.VMEM((D,), BF16),
            pltpu.VMEM((D,), BF16),
            pltpu.VMEM((D,), BF16),
            pltpu.VMEM((1, HD), F32),
            pltpu.VMEM((GROUP * HD,), BF16),
            pltpu.VMEM((HD,), BF16),
            pltpu.VMEM((HD,), BF16),
            pltpu.VMEM((ROWS, GROUP, HD), F32),
            pltpu.VMEM((ROWS, GROUP, LMAX), F32),
            pltpu.VMEM((ROWS, GROUP, HD), F32),
            pltpu.VMEM((ROWS, GROUP * HD), BF16),
            pltpu.VMEM((ROWS, D), BF16),
            pltpu.VMEM((ROWS, FF), F32),
            pltpu.VMEM((ROWS, FF), F32),
            pltpu.VMEM((ROWS, FF), BF16),
            pltpu.VMEM((2, ROWS, CHUNK), F32),
            pltpu.VMEM((2, CHUNK, ROWS), F32),
            pltpu.VMEM((2, NDEV, ROWS, COL), BF16),
            pltpu.VMEM((2, NDEV, ROWS, COL), BF16),
            pltpu.VMEM((2, ROWS, COL), BF16),
            pltpu.VMEM((2, NDEV, ROWS, COL), BF16),
            pltpu.VMEM((8, 128), F32),
            pltpu.VMEM((NDEV, 8, 128), F32),
            DMA((10,)),
            DMA((2,)),
            DMA((SLOTS,)),
            DMA((QUARTERS,)),
            DMA((5,)),
            DMA((5,)),
        ],
        compiler_params=pltpu.CompilerParams(collective_id=0, has_side_effects=True, vmem_limit_bytes=STEP_VMEM),
        name='step',
    )(seq_lens, next_tok, tok_hidden, g_attn, g_mlp, g_final, jnp.asarray(rotary_freqs()), b_q, b_k, b_v,
      w_q, w_k, w_v, k_cache, v_cache, w_o, w_gate, w_up, w_down, w_head)
    y_out, k_out, v_out, logp, lse = pl.pallas_call(
        finish_kernel,
        out_shape=(hidden, cache, cache, vector, vector),
        in_specs=[VM] * 4,
        out_specs=(HB,) * 5,
        scratch_shapes=[
            pltpu.VMEM((ROWS,), F32),
            pltpu.VMEM((ROWS,), F32),
            DMA((5,)),
        ],
        compiler_params=pltpu.CompilerParams(vmem_limit_bytes=2**20),
        name='finish',
    )(y, k_all, v_all, stats)
    shape = (ROWS, LMAX, 1, HD)
    return y_out, k_out.reshape(shape), v_out.reshape(shape), logp, lse


def solution(mesh):
    row_spec = P('dp', None)
    vec_spec = P('dp')
    cache_spec = P('dp', None, 'tp', None)
    col_spec = P(None, 'tp')
    part_spec = P('tp')
    whole_spec = P(None)
    in_specs = (row_spec, vec_spec, cache_spec, cache_spec, vec_spec, whole_spec, col_spec, part_spec, col_spec, part_spec, col_spec, part_spec, P('tp', None), whole_spec, col_spec, col_spec, P('tp', None), whole_spec, P('tp', None))
    out_specs = (row_spec, cache_spec, cache_spec, vec_spec, vec_spec)
    return jax.shard_map(local_step, mesh=mesh, in_specs=in_specs, out_specs=out_specs, check_vma=False)
```

```python
import functools

import jax
import jax.numpy as jnp
import numpy as np
from jax import lax
from jax.experimental import pallas as pl
from jax.experimental.pallas import tpu as pltpu
from jax.sharding import PartitionSpec as P

THETA = 1000000.0
EPS = 1e-6
F32 = jnp.float32
BF16 = jnp.bfloat16
ROWS = 16
D = 4096
HD = 128
GROUP = 4
LMAX = 512
FF = 1792
VOC = 16032
COL = 512
NDEV = 8
SLOTS = 12
CHUNK = 512
DEEP = 256
WO = 2
GU0 = 3
DN0 = 11
HEAD0 = 15
NFULL = VOC // CHUNK
REST = VOC - NFULL * CHUNK
PAIRS = NFULL // 2
PIECES = ((0, 2048), (2048, 3072), (3072, 4096))
STEP_VMEM = 56 * 2**20

NT_DIMS = (((1,), (1,)), ((), ()))
NN_DIMS = (((1,), (0,)), ((), ()))


def mm(lhs, rhs, dims=NN_DIMS):
    return lax.dot_general(lhs, rhs, dims, preferred_element_type=F32)


def row_vector(scalars_ref, dtype, shape, axis):
    ids = lax.broadcasted_iota(jnp.int32, shape, axis)
    vec = jnp.zeros(shape, dtype)
    for row in range(ROWS):
        vec = jnp.where(ids == row, scalars_ref[row].astype(dtype), vec)
    return vec


def flip(me, k):
    out = 0
    for bit in (1, 2, 4):
        mine = lax.rem(me // bit, 2)
        out = out + bit * ((1 - mine) if k & bit else mine)
    return out


def norm_cols(parts_ref, gain, out_ref):
    total = jnp.zeros((ROWS, 1), F32)
    for j in range(NDEV):
        part = parts_ref[j].astype(F32)
        total = total + jnp.sum(part * part, axis=-1, keepdims=True)
    inv = lax.rsqrt(total * (1.0 / D) + EPS)
    for j in range(NDEV):
        cols = slice(j * COL, (j + 1) * COL)
        out_ref[:, cols] = (parts_ref[j].astype(F32) * inv * gain[:, cols]).astype(BF16)


def step_kernel(lens_hbm, tok_hbm, x_hbm, ga_hbm, gm_hbm, gf_hbm, freq_hbm, bq_hbm, bk_hbm, bv_hbm,
                wq_hbm, wk_hbm, wv_hbm, kc_hbm, vc_hbm, wo_hbm, wg_hbm, wu_hbm, wd_hbm, wh_hbm,
                y_ref, k_ref, v_ref, st_ref,
                ring, lens_ref, tok_ref, x_buf, ga_ref, gm_ref, gf_ref, freq_ref, bq_ref, bk_ref, bv_ref,
                q_scr, s_scr, o_scr, obuf,
                mbuf, gacc, uacc, hbuf, za_buf, zb_buf, rs_send, rs_recv, own, gath, st_send, st_recv,
                small_sems, cache_sems, ring_sems, last_sems, send_sems, recv_sems):
    me = lax.axis_index('tp')
    peers = {k: flip(me, k) for k in range(1, NDEV)}
    order = (7, 6, 5, 4, 3, 2, 1)
    copy = pltpu.make_async_copy

    def fetch(c):
        slot, sem = ring.at[c % SLOTS], ring_sems.at[c % SLOTS]
        blocks = [pl.ds(j * CHUNK, CHUNK) for j in range(D // CHUNK)]
        if c == 0:
            return [copy(wq_hbm.at[rows, :], slot.at[:, j * COL:(j + 1) * COL], sem) for j, rows in enumerate(blocks)]
        if c == 1:
            return [copy(src.at[rows, :], slot.at[:, (2 * j + i) * HD:(2 * j + i + 1) * HD], sem)
                    for j, rows in enumerate(blocks) for i, src in enumerate((wk_hbm, wv_hbm))]
        if c == WO:
            return [copy(wo_hbm, slot, sem)]
        if c < DN0:
            rows = pl.ds((c - GU0) * CHUNK, CHUNK)
            return [copy(wg_hbm.at[rows, :], slot.at[:, 0:FF], sem),
                    copy(wu_hbm.at[rows, :], slot.at[:, FF:2 * FF], sem)]
        first = (c - DN0) * CHUNK
        size = min(CHUNK, FF - first)
        return [copy(wd_hbm.at[pl.ds(first, size), :], slot.at[0:size, :], sem)]

    def landed(c):
        width = {0: D, 1: 2 * HD * (D // CHUNK)}.get(c, 2 * FF if GU0 <= c < DN0 else D)
        rows = min(CHUNK, FF - (c - DN0) * CHUNK) if c >= DN0 else CHUNK
        copy(wo_hbm.at[0:rows, 0:width], ring.at[c % SLOTS, 0:rows, 0:width], ring_sems.at[c % SLOTS]).wait()

    def head_slot(h):
        return lax.rem(h + HEAD0, SLOTS)

    def head_row(h):
        return REST + (h - 1) * CHUNK

    def head_rest():
        return copy(wh_hbm.at[0:REST, :], ring.at[HEAD0 % SLOTS, 0:REST, :], ring_sems.at[HEAD0 % SLOTS])

    def head_copy(h):
        slot = head_slot(h)
        return copy(wh_hbm.at[pl.ds(pl.multiple_of(head_row(h), 32), CHUNK), :], ring.at[slot], ring_sems.at[slot])

    def head_pieces(h):
        slot = (h + HEAD0) % SLOTS
        return [copy(wh_hbm.at[pl.ds(head_row(h), CHUNK), lo:hi], ring.at[slot, :, lo:hi], last_sems.at[q])
                for q, (lo, hi) in enumerate(PIECES)]

    def start_chunk(c):
        if c < HEAD0:
            for cp in fetch(c):
                cp.start(priority=0 if c < WO else 1)
        elif c == HEAD0:
            head_rest().start(priority=1)
        else:
            head_copy(c - HEAD0).start(priority=1)

    smalls = [copy(src, dst, small_sems.at[i]) for i, (src, dst) in enumerate((
        (x_hbm, x_buf), (ga_hbm, ga_ref), (lens_hbm, lens_ref), (freq_hbm, freq_ref), (bq_hbm, bq_ref), (bk_hbm, bk_ref),
        (bv_hbm, bv_ref), (gm_hbm, gm_ref), (gf_hbm, gf_ref), (tok_hbm, tok_ref)))]
    for cp in smalls:
        cp.start()
    caches = [copy(kc_hbm, k_ref, cache_sems.at[0]), copy(vc_hbm, v_ref, cache_sems.at[1])]
    for c in range(SLOTS):
        if c == WO:
            for cp in caches:
                cp.start()
        start_chunk(c)
    barrier = pltpu.get_barrier_semaphore()
    for k in order:
        pl.semaphore_signal(barrier, inc=1, device_id={'tp': peers[k]}, device_id_type=pl.DeviceIdType.MESH)

    for cp in smalls:
        cp.wait()
    angles = row_vector(lens_ref, F32, (ROWS, HD), 0) * freq_ref[...]
    cos = jnp.cos(angles)
    lane = lax.broadcasted_iota(jnp.int32, (ROWS, HD), 1)
    sin = jnp.sin(angles)
    sin = jnp.where(lane < HD // 2, -sin, sin)
    xf = x_buf[...].astype(F32)
    inv = lax.rsqrt(jnp.mean(xf * xf, axis=-1, keepdims=True) + EPS)
    normed = (xf * inv * ga_ref[...].astype(F32)[None, :]).astype(BF16)
    landed(0)
    q_proj = bq_ref[...].astype(F32)[None, :]
    for j in range(D // CHUNK):
        q_proj = q_proj + mm(normed[:, j * CHUNK:(j + 1) * CHUNK], ring[0, :, j * COL:(j + 1) * COL])
    start_chunk(SLOTS)
    for h in range(GROUP):
        q_h = q_proj[:, h * HD:(h + 1) * HD]
        q_scr[:, h, :] = (q_h * cos + pltpu.roll(q_h, HD // 2, 1) * sin).astype(BF16).astype(F32)
    landed(1)
    kv_proj = jnp.zeros((ROWS, 2 * HD), F32)
    for j in range(D // CHUNK):
        kv_proj = kv_proj + mm(normed[:, j * CHUNK:(j + 1) * CHUNK], ring[1, :, 2 * j * HD:2 * (j + 1) * HD])
    start_chunk(1 + SLOTS)
    k_proj = kv_proj[:, 0:HD] + bk_ref[...].astype(F32)[None, :]
    k_new = (k_proj * cos + pltpu.roll(k_proj, HD // 2, 1) * sin).astype(BF16)
    v_new = (kv_proj[:, HD:] + bv_ref[...].astype(F32)[None, :]).astype(BF16)

    caches[0].wait()
    slot_ids = lax.broadcasted_iota(jnp.int32, (GROUP, LMAX), 1)
    for b in range(ROWS):
        s_b = mm(q_scr[b].astype(BF16), k_ref[b], NT_DIMS) * (HD ** -0.5)
        s_scr[b] = jnp.where(slot_ids < lens_ref[b], s_b, -jnp.inf)
    s_new = jnp.sum(q_scr[...] * k_new.astype(F32)[:, None, :], axis=-1, keepdims=True) * (HD ** -0.5)
    scores = s_scr[...]
    top = jnp.maximum(jnp.max(scores, axis=-1, keepdims=True), s_new)
    e = jnp.exp(scores - top)
    e_new = jnp.exp(s_new - top)
    denom = jnp.sum(e, axis=-1, keepdims=True) + e_new
    s_scr[...] = e / denom
    p_new = (e_new / denom).astype(BF16).astype(F32)
    caches[1].wait()
    for b in range(ROWS):
        o_scr[b] = mm(s_scr[b].astype(BF16), v_ref[b])
    o_scr[...] += p_new * v_new.astype(F32)[:, None, :]
    for h in range(GROUP):
        obuf[:, h * HD:(h + 1) * HD] = o_scr[:, h, :].astype(BF16)

    pl.semaphore_wait(barrier, NDEV - 1)

    def remote(src, dst, ssem, rsem, k):
        return pltpu.make_async_remote_copy(src_ref=src, dst_ref=dst, send_sem=ssem, recv_sem=rsem,
                                            device_id={'tp': peers[k]}, device_id_type=pl.DeviceIdType.MESH)

    def exchange(phase, payload, landing, size):
        for k in order:
            remote(payload(k), landing(k), send_sems.at[phase], recv_sems.at[phase], k).start()
        return remote(size, size, send_sems.at[phase], recv_sems.at[phase], 1)

    def all_reduce(phase, partial, residual, used, meanwhile):
        def send_part(k):
            rs_send[phase, k] = partial(peers[k]).astype(BF16)
            return rs_send.at[phase, k]

        seven = rs_recv.at[phase, 1:NDEV]
        scatter = exchange(2 * phase, send_part, lambda k: rs_recv.at[phase, k], seven)
        total = partial(me)
        for c in used:
            start_chunk(c + SLOTS)
        meanwhile()
        scatter.wait_recv()
        for k in reversed(order):
            total = total + rs_recv[phase, k].astype(F32)
        mine = (residual.astype(F32) + total).astype(BF16)
        own[phase] = mine
        gath[phase, me] = mine
        gather = exchange(2 * phase + 1, lambda k: own.at[phase], lambda k: gath.at[phase, me], seven)
        gather.wait_recv()
        return [scatter, gather]

    def columns(dev):
        return pl.ds(pl.multiple_of(dev * COL, COL), COL)

    def insert():
        ids = lax.broadcasted_iota(jnp.int32, (LMAX, HD), 0)
        for b in range(ROWS):
            here = ids == lens_ref[b]
            for ref, new in ((k_ref, k_new), (v_ref, v_new)):
                row = jnp.broadcast_to(new[b:b + 1, :].astype(F32), (LMAX, HD))
                ref[b] = jnp.where(here, row, ref[b].astype(F32)).astype(BF16)

    landed(WO)
    sends = all_reduce(0, lambda dev: mm(obuf[...], ring[WO, :, columns(dev)]), x_buf[:, columns(me)], (WO,), insert)
    norm_cols(gath.at[0], gm_ref[...].astype(F32)[None, :], mbuf)

    for j in range(8):
        landed(GU0 + j)
        m_j = mbuf[:, j * CHUNK:(j + 1) * CHUNK]
        g_j = mm(m_j, ring[(GU0 + j) % SLOTS, :, 0:FF])
        u_j = mm(m_j, ring[(GU0 + j) % SLOTS, :, FF:2 * FF])
        if j == 0:
            gacc[...] = g_j
            uacc[...] = u_j
        else:
            gacc[...] += g_j
            uacc[...] += u_j
        start_chunk(GU0 + j + SLOTS)
    gate = gacc[...]
    hbuf[...] = (gate * jax.nn.sigmoid(gate) * uacc[...]).astype(BF16)

    for c in range(DN0, HEAD0):
        landed(c)

    def down(dev):
        total = jnp.zeros((ROWS, COL), F32)
        for j in range(4):
            first, size = j * CHUNK, min(CHUNK, FF - j * CHUNK)
            total = total + mm(hbuf[:, first:first + size], ring[(DN0 + j) % SLOTS, 0:size, columns(dev)])
        return total

    sends += all_reduce(1, down, own[0], range(DN0, HEAD0), lambda: None)
    for j in range(NDEV):
        y_ref[:, j * COL:(j + 1) * COL] = gath[1, j]
    norm_cols(gath.at[1], gf_ref[...].astype(F32)[None, :], mbuf)

    target_row = row_vector(tok_ref, jnp.int32, (1, ROWS), 1) - me * VOC
    target_col = row_vector(tok_ref, jnp.int32, (ROWS, 1), 0) - me * VOC

    def fold(carry, pieces, ids, target):
        top, acc, hit = carry
        new_top = functools.reduce(jnp.maximum, pieces, top)
        acc = acc * jnp.exp(top - new_top)
        for piece, at in zip(pieces, ids):
            acc = acc + jnp.exp(piece - new_top)
            hit = hit + jnp.where(at == target, piece, 0.0)
        return new_top, acc, hit

    def stats_a(z, first, carry):
        ids = lax.broadcasted_iota(jnp.int32, (ROWS, HD), 1) + first
        n = z.shape[1] // HD
        return fold(carry, [z[:, i * HD:(i + 1) * HD] for i in range(n)], [ids + i * HD for i in range(n)], target_col)

    def stats_b(z, first, carry):
        ids = lax.broadcasted_iota(jnp.int32, (8, ROWS), 0) + first
        n = z.shape[0] // 8
        top, acc, hit = carry
        groups = z.reshape(n, 8, ROWS)
        new_top = jnp.maximum(top, jnp.max(groups, axis=0))
        acc = acc * jnp.exp(top - new_top) + jnp.sum(jnp.exp(groups - new_top[None]), axis=0)
        at = lax.broadcasted_iota(jnp.int32, (n, 8, ROWS), 0) * 8 + ids[None]
        hit = hit + jnp.sum(jnp.where(at == target_row[None], groups, 0.0), axis=0)
        return new_top, acc, hit

    def score(sa, sb, size_b, first, last, sums):
        sums = list(sums)
        for k in range(first, last, DEEP):
            f_k = mbuf[:, k:k + DEEP]
            for i, q in enumerate(range(0, CHUNK, DEEP)):
                sums[2 * i] = sums[2 * i] + mm(f_k, ring[sa, q:q + DEEP, k:k + DEEP], NT_DIMS)
                if q < size_b:
                    end = min(q + DEEP, size_b)
                    sums[2 * i + 1] = sums[2 * i + 1] + mm(ring[sb, q:end, k:k + DEEP], f_k, NT_DIMS)
        return sums

    def zeros(size_b):
        sums = []
        for q in range(0, CHUNK, DEEP):
            sums += [jnp.zeros((ROWS, DEEP), F32), jnp.zeros((min(DEEP, size_b - q), ROWS), F32) if q < size_b else None]
        return sums

    def empty(shape):
        return jnp.full(shape, -jnp.inf, F32), jnp.zeros(shape, F32), jnp.zeros(shape, F32)

    def keep(sums, now):
        for i, q in enumerate(range(0, CHUNK, DEEP)):
            za_buf[now, :, q:q + DEEP] = sums[2 * i]
            zb_buf[now, q:q + DEEP, :] = sums[2 * i + 1]

    def stats(now, h, carry):
        return stats_a(za_buf[now], head_row(h), carry[0]), stats_b(zb_buf[now], head_row(h + 1), carry[1])

    def refill(h):
        @pl.when(h + SLOTS < 2 * PAIRS)
        def _():
            head_copy(h + SLOTS).start(priority=1)

    head_rest().wait()
    head_copy(1).wait()
    sums = score(head_slot(1), HEAD0 % SLOTS, REST, 0, D, zeros(REST))
    ca = stats_a(sums[0], head_row(1), empty((ROWS, HD)))
    carry = (stats_a(sums[2], head_row(1) + DEEP, ca), stats_b(sums[1], 0, empty((8, ROWS))))
    for h in (0, 1):
        head_copy(h + SLOTS).start(priority=1)

    def pair(i, carry, first=False):
        h = 2 * i
        head_copy(h).wait()
        head_copy(h + 1).wait()
        sums = score(head_slot(h), head_slot(h + 1), CHUNK, 0, D, zeros(CHUNK))
        if not first:
            carry = stats(lax.rem(i - 1, 2), h - 2, carry)
        keep(sums, lax.rem(i, 2))
        refill(h)
        refill(h + 1)

        @pl.when(h + SLOTS == 2 * PAIRS)
        def _():
            for pieces in zip(last_a, last_b):
                for cp in pieces:
                    cp.start(priority=1)
        return carry

    last_a, last_b = head_pieces(2 * PAIRS), head_pieces(2 * PAIRS + 1)
    carry = pair(1, carry, True)
    carry = lax.fori_loop(2, PAIRS, pair, carry)
    sums = zeros(CHUNK)
    for q, (lo, hi) in enumerate(PIECES):
        width = 2 * (hi - lo)
        copy(wo_hbm.at[:, 0:width], ring.at[0, :, 0:width], last_sems.at[q]).wait()
        sums = score((2 * PAIRS + HEAD0) % SLOTS, (2 * PAIRS + 1 + HEAD0) % SLOTS, CHUNK, lo, hi, sums)
        if q == 0:
            carry = stats((PAIRS - 1) % 2, 2 * PAIRS - 2, carry)
    ca, cb = carry
    for i, q in enumerate(range(0, CHUNK, DEEP)):
        ca = stats_a(sums[2 * i], head_row(2 * PAIRS) + q, ca)
        cb = stats_b(sums[2 * i + 1], head_row(2 * PAIRS + 1) + q, cb)

    eye = lax.broadcasted_iota(jnp.int32, (ROWS, ROWS), 0) == lax.broadcasted_iota(jnp.int32, (ROWS, ROWS), 1)

    def as_row(col):
        return jnp.sum(jnp.where(eye, jnp.broadcast_to(col, (ROWS, ROWS)), 0.0), axis=0, keepdims=True)

    top_a = jnp.max(ca[0], axis=1, keepdims=True)
    acc_a = as_row(jnp.sum(ca[1] * jnp.exp(ca[0] - top_a), axis=1, keepdims=True))
    hit_a = as_row(jnp.sum(ca[2], axis=1, keepdims=True))
    top_a = as_row(top_a)
    top_b = jnp.max(cb[0], axis=0, keepdims=True)
    acc_b = jnp.sum(cb[1] * jnp.exp(cb[0] - top_b), axis=0, keepdims=True)
    hit_b = jnp.sum(cb[2], axis=0, keepdims=True)
    top = jnp.maximum(top_a, top_b)
    acc = acc_a * jnp.exp(top_a - top) + acc_b * jnp.exp(top_b - top)
    hit = hit_a + hit_b
    st_send[0:1, 0:ROWS] = top
    st_send[1:2, 0:ROWS] = acc
    st_send[2:3, 0:ROWS] = hit
    share = exchange(4, lambda k: st_send, lambda k: st_recv.at[k], st_recv.at[1:NDEV])
    share.wait_recv()
    tops, accs, hits = [top], [acc], [hit]
    for k in reversed(order):
        tops.append(st_recv[k, 0:1, 0:ROWS])
        accs.append(st_recv[k, 1:2, 0:ROWS])
        hits.append(st_recv[k, 2:3, 0:ROWS])
    best = functools.reduce(jnp.maximum, tops)
    exp_sum = sum(a * jnp.exp(t - best) for t, a in zip(tops, accs))
    lse = best + jnp.log(exp_sum)
    st_ref[0:1, 0:ROWS] = sum(hits) - lse
    st_ref[1:2, 0:ROWS] = lse
    for group in sends + [share]:
        group.wait_send()


def finish_kernel(y_ref, k_ref, v_ref, st_ref, y_hbm, k_hbm, v_hbm, logp_hbm, lse_hbm, logp_ref, lse_ref, sems):
    logp_ref[...] = st_ref[0, 0:ROWS]
    lse_ref[...] = st_ref[1, 0:ROWS]
    copies = [pltpu.make_async_copy(src, dst, sems.at[i]) for i, (src, dst) in enumerate((
        (k_ref, k_hbm), (v_ref, v_hbm), (y_ref, y_hbm), (logp_ref, logp_hbm), (lse_ref, lse_hbm)))]
    for cp in copies:
        cp.start()
    for cp in copies:
        cp.wait()


def rotary_freqs():
    half = HD // 2
    freq = np.power(THETA, np.arange(half) * (-2.0 / HD)).astype(np.float32)
    return np.concatenate([freq, freq])[None, :]


VM = pl.BlockSpec(memory_space=pltpu.VMEM)
HB = pl.BlockSpec(memory_space=pl.ANY)
DMA = pltpu.SemaphoreType.DMA


def local_step(tok_hidden, seq_lens, k_cache, v_cache, next_tok, g_attn, w_q, b_q, w_k, b_k, w_v, b_v, w_o, g_mlp, w_gate, w_up, w_down, g_final, w_head):
    k_cache = k_cache.reshape(ROWS, LMAX, HD)
    v_cache = v_cache.reshape(ROWS, LMAX, HD)
    hidden = jax.ShapeDtypeStruct((ROWS, D), BF16)
    cache = jax.ShapeDtypeStruct((ROWS, LMAX, HD), BF16)
    vector = jax.ShapeDtypeStruct((ROWS,), F32)
    y, k_all, v_all, stats = pl.pallas_call(
        step_kernel,
        out_shape=(pltpu.VMEM((ROWS, D), BF16), pltpu.VMEM((ROWS, LMAX, HD), BF16), pltpu.VMEM((ROWS, LMAX, HD), BF16),
                   pltpu.VMEM((8, 128), F32)),
        in_specs=[HB] * 20,
        out_specs=(VM,) * 4,
        scratch_shapes=[
            pltpu.VMEM((SLOTS, CHUNK, D), BF16),
            pltpu.SMEM((ROWS,), jnp.int32),
            pltpu.SMEM((ROWS,), jnp.int32),
            pltpu.VMEM((ROWS, D), BF16),
            pltpu.VMEM((D,), BF16),
            pltpu.VMEM((D,), BF16),
            pltpu.VMEM((D,), BF16),
            pltpu.VMEM((1, HD), F32),
            pltpu.VMEM((GROUP * HD,), BF16),
            pltpu.VMEM((HD,), BF16),
            pltpu.VMEM((HD,), BF16),
            pltpu.VMEM((ROWS, GROUP, HD), F32),
            pltpu.VMEM((ROWS, GROUP, LMAX), F32),
            pltpu.VMEM((ROWS, GROUP, HD), F32),
            pltpu.VMEM((ROWS, GROUP * HD), BF16),
            pltpu.VMEM((ROWS, D), BF16),
            pltpu.VMEM((ROWS, FF), F32),
            pltpu.VMEM((ROWS, FF), F32),
            pltpu.VMEM((ROWS, FF), BF16),
            pltpu.VMEM((2, ROWS, CHUNK), F32),
            pltpu.VMEM((2, CHUNK, ROWS), F32),
            pltpu.VMEM((2, NDEV, ROWS, COL), BF16),
            pltpu.VMEM((2, NDEV, ROWS, COL), BF16),
            pltpu.VMEM((2, ROWS, COL), BF16),
            pltpu.VMEM((2, NDEV, ROWS, COL), BF16),
            pltpu.VMEM((8, 128), F32),
            pltpu.VMEM((NDEV, 8, 128), F32),
            DMA((10,)),
            DMA((2,)),
            DMA((SLOTS,)),
            DMA((len(PIECES),)),
            DMA((5,)),
            DMA((5,)),
        ],
        compiler_params=pltpu.CompilerParams(collective_id=0, has_side_effects=True, vmem_limit_bytes=STEP_VMEM),
        name='step',
    )(seq_lens, next_tok, tok_hidden, g_attn, g_mlp, g_final, jnp.asarray(rotary_freqs()), b_q, b_k, b_v,
      w_q, w_k, w_v, k_cache, v_cache, w_o, w_gate, w_up, w_down, w_head)
    y_out, k_out, v_out, logp, lse = pl.pallas_call(
        finish_kernel,
        out_shape=(hidden, cache, cache, vector, vector),
        in_specs=[VM] * 4,
        out_specs=(HB,) * 5,
        scratch_shapes=[
            pltpu.VMEM((ROWS,), F32),
            pltpu.VMEM((ROWS,), F32),
            DMA((5,)),
        ],
        compiler_params=pltpu.CompilerParams(vmem_limit_bytes=2**20),
        name='finish',
    )(y, k_all, v_all, stats)
    shape = (ROWS, LMAX, 1, HD)
    return y_out, k_out.reshape(shape), v_out.reshape(shape), logp, lse


def solution(mesh):
    row_spec = P('dp', None)
    vec_spec = P('dp')
    cache_spec = P('dp', None, 'tp', None)
    col_spec = P(None, 'tp')
    part_spec = P('tp')
    whole_spec = P(None)
    in_specs = (row_spec, vec_spec, cache_spec, cache_spec, vec_spec, whole_spec, col_spec, part_spec, col_spec, part_spec, col_spec, part_spec, P('tp', None), whole_spec, col_spec, col_spec, P('tp', None), whole_spec, P('tp', None))
    out_specs = (row_spec, cache_spec, cache_spec, vec_spec, vec_spec)
    return jax.shard_map(local_step, mesh=mesh, in_specs=in_specs, out_specs=out_specs, check_vma=False)
```

```python
import functools

import jax
import jax.numpy as jnp
import numpy as np
from jax import lax
from jax.experimental import pallas as pl
from jax.experimental.pallas import tpu as pltpu
from jax.sharding import PartitionSpec as P

THETA = 1000000.0
EPS = 1e-6
F32 = jnp.float32
BF16 = jnp.bfloat16
ROWS = 16
D = 4096
HD = 128
GROUP = 4
LMAX = 512
FF = 1792
VOC = 16032
COL = 512
NDEV = 8
SLOTS = 10
CHUNK = 512
DEEP = 256
WO = 2
GU0 = 3
DN0 = 11
HEAD0 = 15
NFULL = VOC // CHUNK
REST = VOC - NFULL * CHUNK
PAIRS = NFULL // 2
PIECES = ((0, 2048), (2048, 3072), (3072, 4096))
STEP_VMEM = 50 * 2**20

NT_DIMS = (((1,), (1,)), ((), ()))
NN_DIMS = (((1,), (0,)), ((), ()))


def mm(lhs, rhs, dims=NN_DIMS):
    return lax.dot_general(lhs, rhs, dims, preferred_element_type=F32)


def row_vector(scalars_ref, dtype, shape, axis):
    ids = lax.broadcasted_iota(jnp.int32, shape, axis)
    vec = jnp.zeros(shape, dtype)
    for row in range(ROWS):
        vec = jnp.where(ids == row, scalars_ref[row].astype(dtype), vec)
    return vec


def flip(me, k):
    out = 0
    for bit in (1, 2, 4):
        mine = lax.rem(me // bit, 2)
        out = out + bit * ((1 - mine) if k & bit else mine)
    return out


def norm_cols(parts_ref, gain, out_ref):
    total = jnp.zeros((ROWS, 1), F32)
    for j in range(NDEV):
        part = parts_ref[j].astype(F32)
        total = total + jnp.sum(part * part, axis=-1, keepdims=True)
    inv = lax.rsqrt(total * (1.0 / D) + EPS)
    for j in range(NDEV):
        cols = slice(j * COL, (j + 1) * COL)
        out_ref[:, cols] = (parts_ref[j].astype(F32) * inv * gain[:, cols]).astype(BF16)


def step_kernel(lens_hbm, tok_hbm, x_hbm, ga_hbm, gm_hbm, gf_hbm, freq_hbm, bq_hbm, bk_hbm, bv_hbm,
                wq_hbm, wk_hbm, wv_hbm, kc_hbm, vc_hbm, wo_hbm, wg_hbm, wu_hbm, wd_hbm, wh_hbm,
                y_ref, k_ref, v_ref, st_ref,
                ring, lens_ref, tok_ref, x_buf, ga_ref, gm_ref, gf_ref, freq_ref, bq_ref, bk_ref, bv_ref,
                q_scr, s_scr, o_scr, obuf,
                mbuf, gacc, uacc, hbuf, za_buf, zb_buf, rs_send, rs_recv, own, gath, st_send, st_recv,
                small_sems, cache_sems, ring_sems, send_sems, recv_sems):
    me = lax.axis_index('tp')
    peers = {k: flip(me, k) for k in range(1, NDEV)}
    order = (7, 6, 5, 4, 3, 2, 1)
    copy = pltpu.make_async_copy

    def fetch(c):
        slot, sem = ring.at[c % SLOTS], ring_sems.at[c % SLOTS]
        blocks = [pl.ds(j * CHUNK, CHUNK) for j in range(D // CHUNK)]
        if c == 0:
            return [copy(wq_hbm.at[rows, :], slot.at[:, j * COL:(j + 1) * COL], sem) for j, rows in enumerate(blocks)]
        if c == 1:
            return [copy(src.at[rows, :], slot.at[:, (2 * j + i) * HD:(2 * j + i + 1) * HD], sem)
                    for j, rows in enumerate(blocks) for i, src in enumerate((wk_hbm, wv_hbm))]
        if c == WO:
            return [copy(wo_hbm, slot, sem)]
        if c < DN0:
            rows = pl.ds((c - GU0) * CHUNK, CHUNK)
            return [copy(wg_hbm.at[rows, :], slot.at[:, 0:FF], sem),
                    copy(wu_hbm.at[rows, :], slot.at[:, FF:2 * FF], sem)]
        first = (c - DN0) * CHUNK
        size = min(CHUNK, FF - first)
        return [copy(wd_hbm.at[pl.ds(first, size), :], slot.at[0:size, :], sem)]

    def landed(c):
        width = {0: D, 1: 2 * HD * (D // CHUNK)}.get(c, 2 * FF if GU0 <= c < DN0 else D)
        rows = min(CHUNK, FF - (c - DN0) * CHUNK) if c >= DN0 else CHUNK
        copy(wo_hbm.at[0:rows, 0:width], ring.at[c % SLOTS, 0:rows, 0:width], ring_sems.at[c % SLOTS]).wait()

    def head_slot(h):
        return lax.rem(h + HEAD0, SLOTS)

    def head_row(h):
        return REST + (h - 1) * CHUNK

    def head_rest():
        return copy(wh_hbm.at[0:REST, :], ring.at[HEAD0 % SLOTS, 0:REST, :], ring_sems.at[HEAD0 % SLOTS])

    def head_copy(h):
        slot = head_slot(h)
        return copy(wh_hbm.at[pl.ds(pl.multiple_of(head_row(h), 32), CHUNK), :], ring.at[slot], ring_sems.at[slot])

    def head_pieces(h):
        slot = (h + HEAD0) % SLOTS
        return [copy(wh_hbm.at[pl.ds(head_row(h), CHUNK), lo:hi], ring.at[slot, :, lo:hi], small_sems.at[q])
                for q, (lo, hi) in enumerate(PIECES)]

    def start_chunk(c):
        if c < HEAD0:
            for cp in fetch(c):
                cp.start(priority=0 if c < WO else 1)
        elif c == HEAD0:
            head_rest().start(priority=1)
        else:
            head_copy(c - HEAD0).start(priority=1)

    smalls = [copy(src, dst, small_sems.at[i]) for i, (src, dst) in enumerate((
        (x_hbm, x_buf), (ga_hbm, ga_ref), (lens_hbm, lens_ref), (freq_hbm, freq_ref), (bq_hbm, bq_ref), (bk_hbm, bk_ref),
        (bv_hbm, bv_ref), (gm_hbm, gm_ref), (gf_hbm, gf_ref), (tok_hbm, tok_ref)))]
    for cp in smalls:
        cp.start()
    caches = [copy(kc_hbm, k_ref, cache_sems.at[0]), copy(vc_hbm, v_ref, cache_sems.at[1])]
    for c in range(SLOTS):
        if c == WO:
            for cp in caches:
                cp.start()
        start_chunk(c)
    barrier = pltpu.get_barrier_semaphore()
    for k in order:
        pl.semaphore_signal(barrier, inc=1, device_id={'tp': peers[k]}, device_id_type=pl.DeviceIdType.MESH)

    for cp in smalls:
        cp.wait()
    angles = row_vector(lens_ref, F32, (ROWS, HD), 0) * freq_ref[...]
    cos = jnp.cos(angles)
    lane = lax.broadcasted_iota(jnp.int32, (ROWS, HD), 1)
    sin = jnp.sin(angles)
    sin = jnp.where(lane < HD // 2, -sin, sin)
    xf = x_buf[...].astype(F32)
    inv = lax.rsqrt(jnp.mean(xf * xf, axis=-1, keepdims=True) + EPS)
    normed = (xf * inv * ga_ref[...].astype(F32)[None, :]).astype(BF16)
    landed(0)
    q_proj = bq_ref[...].astype(F32)[None, :]
    for j in range(D // CHUNK):
        q_proj = q_proj + mm(normed[:, j * CHUNK:(j + 1) * CHUNK], ring[0, :, j * COL:(j + 1) * COL])
    start_chunk(SLOTS)
    for h in range(GROUP):
        q_h = q_proj[:, h * HD:(h + 1) * HD]
        q_scr[:, h, :] = (q_h * cos + pltpu.roll(q_h, HD // 2, 1) * sin).astype(BF16).astype(F32)
    landed(1)
    kv_proj = jnp.zeros((ROWS, 2 * HD), F32)
    for j in range(D // CHUNK):
        kv_proj = kv_proj + mm(normed[:, j * CHUNK:(j + 1) * CHUNK], ring[1, :, 2 * j * HD:2 * (j + 1) * HD])
    start_chunk(1 + SLOTS)
    k_proj = kv_proj[:, 0:HD] + bk_ref[...].astype(F32)[None, :]
    k_new = (k_proj * cos + pltpu.roll(k_proj, HD // 2, 1) * sin).astype(BF16)
    v_new = (kv_proj[:, HD:] + bv_ref[...].astype(F32)[None, :]).astype(BF16)

    caches[0].wait()
    slot_ids = lax.broadcasted_iota(jnp.int32, (GROUP, LMAX), 1)
    for b in range(ROWS):
        s_b = mm(q_scr[b].astype(BF16), k_ref[b], NT_DIMS) * (HD ** -0.5)
        s_scr[b] = jnp.where(slot_ids < lens_ref[b], s_b, -jnp.inf)
    s_new = jnp.sum(q_scr[...] * k_new.astype(F32)[:, None, :], axis=-1, keepdims=True) * (HD ** -0.5)
    scores = s_scr[...]
    top = jnp.maximum(jnp.max(scores, axis=-1, keepdims=True), s_new)
    e = jnp.exp(scores - top)
    e_new = jnp.exp(s_new - top)
    denom = jnp.sum(e, axis=-1, keepdims=True) + e_new
    s_scr[...] = e / denom
    p_new = (e_new / denom).astype(BF16).astype(F32)
    caches[1].wait()
    for b in range(ROWS):
        o_scr[b] = mm(s_scr[b].astype(BF16), v_ref[b])
    o_scr[...] += p_new * v_new.astype(F32)[:, None, :]
    for h in range(GROUP):
        obuf[:, h * HD:(h + 1) * HD] = o_scr[:, h, :].astype(BF16)

    pl.semaphore_wait(barrier, NDEV - 1)

    def remote(src, dst, ssem, rsem, k):
        return pltpu.make_async_remote_copy(src_ref=src, dst_ref=dst, send_sem=ssem, recv_sem=rsem,
                                            device_id={'tp': peers[k]}, device_id_type=pl.DeviceIdType.MESH)

    def exchange(phase, payload, landing, size):
        for k in order:
            remote(payload(k), landing(k), send_sems.at[phase % 2], recv_sems.at[phase], k).start()
        return remote(size, size, send_sems.at[phase % 2], recv_sems.at[phase], 1)

    def all_reduce(phase, partial, residual, used, meanwhile):
        def send_part(k):
            rs_send[phase, k] = partial(peers[k]).astype(BF16)
            return rs_send.at[phase, k]

        seven = rs_recv.at[phase, 1:NDEV]
        scatter = exchange(2 * phase, send_part, lambda k: rs_recv.at[phase, k], seven)
        total = partial(me)
        for c in used:
            start_chunk(c + SLOTS)
        meanwhile()
        scatter.wait_recv()
        for k in reversed(order):
            total = total + rs_recv[phase, k].astype(F32)
        mine = (residual.astype(F32) + total).astype(BF16)
        own[phase] = mine
        gath[phase, me] = mine
        gather = exchange(2 * phase + 1, lambda k: own.at[phase], lambda k: gath.at[phase, me], seven)
        gather.wait_recv()
        return [scatter, gather]

    def columns(dev):
        return pl.ds(pl.multiple_of(dev * COL, COL), COL)

    def insert():
        ids = lax.broadcasted_iota(jnp.int32, (LMAX, HD), 0)
        for b in range(ROWS):
            here = ids == lens_ref[b]
            for ref, new in ((k_ref, k_new), (v_ref, v_new)):
                row = jnp.broadcast_to(new[b:b + 1, :].astype(F32), (LMAX, HD))
                ref[b] = jnp.where(here, row, ref[b].astype(F32)).astype(BF16)

    landed(WO)
    sends = all_reduce(0, lambda dev: mm(obuf[...], ring[WO, :, columns(dev)]), x_buf[:, columns(me)], (WO,), insert)
    norm_cols(gath.at[0], gm_ref[...].astype(F32)[None, :], mbuf)

    for j in range(8):
        landed(GU0 + j)
        m_j = mbuf[:, j * CHUNK:(j + 1) * CHUNK]
        g_j = mm(m_j, ring[(GU0 + j) % SLOTS, :, 0:FF])
        u_j = mm(m_j, ring[(GU0 + j) % SLOTS, :, FF:2 * FF])
        if j == 0:
            gacc[...] = g_j
            uacc[...] = u_j
        else:
            gacc[...] += g_j
            uacc[...] += u_j
        start_chunk(GU0 + j + SLOTS)
    gate = gacc[...]
    hbuf[...] = (gate * jax.nn.sigmoid(gate) * uacc[...]).astype(BF16)

    for c in range(DN0, HEAD0):
        landed(c)

    def down(dev):
        total = jnp.zeros((ROWS, COL), F32)
        for j in range(4):
            first, size = j * CHUNK, min(CHUNK, FF - j * CHUNK)
            total = total + mm(hbuf[:, first:first + size], ring[(DN0 + j) % SLOTS, 0:size, columns(dev)])
        return total

    for group in sends:
        group.wait_send()
    sends = all_reduce(1, down, own[0], range(DN0, HEAD0), lambda: None)
    for j in range(NDEV):
        y_ref[:, j * COL:(j + 1) * COL] = gath[1, j]
    norm_cols(gath.at[1], gf_ref[...].astype(F32)[None, :], mbuf)

    target_row = row_vector(tok_ref, jnp.int32, (1, ROWS), 1) - me * VOC
    target_col = row_vector(tok_ref, jnp.int32, (ROWS, 1), 0) - me * VOC

    def fold(carry, pieces, ids, target):
        top, acc, hit = carry
        new_top = functools.reduce(jnp.maximum, pieces, top)
        acc = acc * jnp.exp(top - new_top)
        for piece, at in zip(pieces, ids):
            acc = acc + jnp.exp(piece - new_top)
            hit = hit + jnp.where(at == target, piece, 0.0)
        return new_top, acc, hit

    def stats_a(z, first, carry):
        ids = lax.broadcasted_iota(jnp.int32, (ROWS, HD), 1) + first
        n = z.shape[1] // HD
        return fold(carry, [z[:, i * HD:(i + 1) * HD] for i in range(n)], [ids + i * HD for i in range(n)], target_col)

    def stats_b(z, first, carry):
        ids = lax.broadcasted_iota(jnp.int32, (8, ROWS), 0) + first
        n = z.shape[0] // 8
        top, acc, hit = carry
        groups = z.reshape(n, 8, ROWS)
        new_top = jnp.maximum(top, jnp.max(groups, axis=0))
        acc = acc * jnp.exp(top - new_top) + jnp.sum(jnp.exp(groups - new_top[None]), axis=0)
        at = lax.broadcasted_iota(jnp.int32, (n, 8, ROWS), 0) * 8 + ids[None]
        hit = hit + jnp.sum(jnp.where(at == target_row[None], groups, 0.0), axis=0)
        return new_top, acc, hit

    def score(sa, sb, size_b, first, last, sums):
        sums = list(sums)
        for k in range(first, last, DEEP):
            f_k = mbuf[:, k:k + DEEP]
            for i, q in enumerate(range(0, CHUNK, DEEP)):
                sums[2 * i] = sums[2 * i] + mm(f_k, ring[sa, q:q + DEEP, k:k + DEEP], NT_DIMS)
                if q < size_b:
                    end = min(q + DEEP, size_b)
                    sums[2 * i + 1] = sums[2 * i + 1] + mm(ring[sb, q:end, k:k + DEEP], f_k, NT_DIMS)
        return sums

    def zeros(size_b):
        sums = []
        for q in range(0, CHUNK, DEEP):
            sums += [jnp.zeros((ROWS, DEEP), F32), jnp.zeros((min(DEEP, size_b - q), ROWS), F32) if q < size_b else None]
        return sums

    def empty(shape):
        return jnp.full(shape, -jnp.inf, F32), jnp.zeros(shape, F32), jnp.zeros(shape, F32)

    def keep(sums, now):
        for i, q in enumerate(range(0, CHUNK, DEEP)):
            za_buf[now, :, q:q + DEEP] = sums[2 * i]
            zb_buf[now, q:q + DEEP, :] = sums[2 * i + 1]

    def stats(now, h, carry):
        return stats_a(za_buf[now], head_row(h), carry[0]), stats_b(zb_buf[now], head_row(h + 1), carry[1])

    def refill(h):
        @pl.when(h + SLOTS < 2 * PAIRS)
        def _():
            head_copy(h + SLOTS).start(priority=1)

    head_rest().wait()
    head_copy(1).wait()
    sums = score(head_slot(1), HEAD0 % SLOTS, REST, 0, D, zeros(REST))
    ca = stats_a(sums[0], head_row(1), empty((ROWS, HD)))
    carry = (stats_a(sums[2], head_row(1) + DEEP, ca), stats_b(sums[1], 0, empty((8, ROWS))))
    for h in (0, 1):
        head_copy(h + SLOTS).start(priority=1)

    def pair(i, carry, first=False):
        h = 2 * i
        head_copy(h).wait()
        head_copy(h + 1).wait()
        sums = score(head_slot(h), head_slot(h + 1), CHUNK, 0, D, zeros(CHUNK))
        if not first:
            carry = stats(lax.rem(i - 1, 2), h - 2, carry)
        keep(sums, lax.rem(i, 2))
        refill(h)
        refill(h + 1)

        @pl.when(h + SLOTS == 2 * PAIRS)
        def _():
            for pieces in zip(last_a, last_b):
                for cp in pieces:
                    cp.start(priority=1)
        return carry

    last_a, last_b = head_pieces(2 * PAIRS), head_pieces(2 * PAIRS + 1)
    carry = pair(1, carry, True)
    carry = lax.fori_loop(2, PAIRS, pair, carry)
    sums = zeros(CHUNK)
    for q, (lo, hi) in enumerate(PIECES):
        width = 2 * (hi - lo)
        copy(wo_hbm.at[:, 0:width], ring.at[0, :, 0:width], small_sems.at[q]).wait()
        sums = score((2 * PAIRS + HEAD0) % SLOTS, (2 * PAIRS + 1 + HEAD0) % SLOTS, CHUNK, lo, hi, sums)
        if q == 0:
            carry = stats((PAIRS - 1) % 2, 2 * PAIRS - 2, carry)
    ca, cb = carry
    for i, q in enumerate(range(0, CHUNK, DEEP)):
        ca = stats_a(sums[2 * i], head_row(2 * PAIRS) + q, ca)
        cb = stats_b(sums[2 * i + 1], head_row(2 * PAIRS + 1) + q, cb)

    eye = lax.broadcasted_iota(jnp.int32, (ROWS, ROWS), 0) == lax.broadcasted_iota(jnp.int32, (ROWS, ROWS), 1)

    def as_row(col):
        return jnp.sum(jnp.where(eye, jnp.broadcast_to(col, (ROWS, ROWS)), 0.0), axis=0, keepdims=True)

    top_a = jnp.max(ca[0], axis=1, keepdims=True)
    acc_a = as_row(jnp.sum(ca[1] * jnp.exp(ca[0] - top_a), axis=1, keepdims=True))
    hit_a = as_row(jnp.sum(ca[2], axis=1, keepdims=True))
    top_a = as_row(top_a)
    top_b = jnp.max(cb[0], axis=0, keepdims=True)
    acc_b = jnp.sum(cb[1] * jnp.exp(cb[0] - top_b), axis=0, keepdims=True)
    hit_b = jnp.sum(cb[2], axis=0, keepdims=True)
    top = jnp.maximum(top_a, top_b)
    acc = acc_a * jnp.exp(top_a - top) + acc_b * jnp.exp(top_b - top)
    hit = hit_a + hit_b
    st_send[0:1, 0:ROWS] = top
    st_send[1:2, 0:ROWS] = acc
    st_send[2:3, 0:ROWS] = hit
    for group in sends:
        group.wait_send()
    share = exchange(4, lambda k: st_send, lambda k: st_recv.at[k], st_recv.at[1:NDEV])
    share.wait_recv()
    tops, accs, hits = [top], [acc], [hit]
    for k in reversed(order):
        tops.append(st_recv[k, 0:1, 0:ROWS])
        accs.append(st_recv[k, 1:2, 0:ROWS])
        hits.append(st_recv[k, 2:3, 0:ROWS])
    best = functools.reduce(jnp.maximum, tops)
    exp_sum = sum(a * jnp.exp(t - best) for t, a in zip(tops, accs))
    lse = best + jnp.log(exp_sum)
    st_ref[0:1, 0:ROWS] = sum(hits) - lse
    st_ref[1:2, 0:ROWS] = lse
    share.wait_send()


def finish_kernel(y_ref, k_ref, v_ref, st_ref, y_hbm, k_hbm, v_hbm, logp_hbm, lse_hbm, logp_ref, lse_ref, sems):
    logp_ref[...] = st_ref[0, 0:ROWS]
    lse_ref[...] = st_ref[1, 0:ROWS]
    copies = [pltpu.make_async_copy(src, dst, sems.at[i]) for i, (src, dst) in enumerate((
        (k_ref, k_hbm), (v_ref, v_hbm), (y_ref, y_hbm), (logp_ref, logp_hbm), (lse_ref, lse_hbm)))]
    for cp in copies:
        cp.start()
    for cp in copies:
        cp.wait()


def rotary_freqs():
    half = HD // 2
    freq = np.power(THETA, np.arange(half) * (-2.0 / HD)).astype(np.float32)
    return np.concatenate([freq, freq])[None, :]


VM = pl.BlockSpec(memory_space=pltpu.VMEM)
HB = pl.BlockSpec(memory_space=pl.ANY)
DMA = pltpu.SemaphoreType.DMA


def local_step(tok_hidden, seq_lens, k_cache, v_cache, next_tok, g_attn, w_q, b_q, w_k, b_k, w_v, b_v, w_o, g_mlp, w_gate, w_up, w_down, g_final, w_head):
    k_cache = k_cache.reshape(ROWS, LMAX, HD)
    v_cache = v_cache.reshape(ROWS, LMAX, HD)
    hidden = jax.ShapeDtypeStruct((ROWS, D), BF16)
    cache = jax.ShapeDtypeStruct((ROWS, LMAX, HD), BF16)
    vector = jax.ShapeDtypeStruct((ROWS,), F32)
    y, k_all, v_all, stats = pl.pallas_call(
        step_kernel,
        out_shape=(pltpu.VMEM((ROWS, D), BF16), pltpu.VMEM((ROWS, LMAX, HD), BF16), pltpu.VMEM((ROWS, LMAX, HD), BF16),
                   pltpu.VMEM((8, 128), F32)),
        in_specs=[HB] * 20,
        out_specs=(VM,) * 4,
        scratch_shapes=[
            pltpu.VMEM((SLOTS, CHUNK, D), BF16),
            pltpu.SMEM((ROWS,), jnp.int32),
            pltpu.SMEM((ROWS,), jnp.int32),
            pltpu.VMEM((ROWS, D), BF16),
            pltpu.VMEM((D,), BF16),
            pltpu.VMEM((D,), BF16),
            pltpu.VMEM((D,), BF16),
            pltpu.VMEM((1, HD), F32),
            pltpu.VMEM((GROUP * HD,), BF16),
            pltpu.VMEM((HD,), BF16),
            pltpu.VMEM((HD,), BF16),
            pltpu.VMEM((ROWS, GROUP, HD), F32),
            pltpu.VMEM((ROWS, GROUP, LMAX), F32),
            pltpu.VMEM((ROWS, GROUP, HD), F32),
            pltpu.VMEM((ROWS, GROUP * HD), BF16),
            pltpu.VMEM((ROWS, D), BF16),
            pltpu.VMEM((ROWS, FF), F32),
            pltpu.VMEM((ROWS, FF), F32),
            pltpu.VMEM((ROWS, FF), BF16),
            pltpu.VMEM((2, ROWS, CHUNK), F32),
            pltpu.VMEM((2, CHUNK, ROWS), F32),
            pltpu.VMEM((2, NDEV, ROWS, COL), BF16),
            pltpu.VMEM((2, NDEV, ROWS, COL), BF16),
            pltpu.VMEM((2, ROWS, COL), BF16),
            pltpu.VMEM((2, NDEV, ROWS, COL), BF16),
            pltpu.VMEM((8, 128), F32),
            pltpu.VMEM((NDEV, 8, 128), F32),
            DMA((10,)),
            DMA((2,)),
            DMA((SLOTS,)),
            DMA((2,)),
            DMA((5,)),
        ],
        compiler_params=pltpu.CompilerParams(collective_id=0, has_side_effects=True, vmem_limit_bytes=STEP_VMEM),
        name='step',
    )(seq_lens, next_tok, tok_hidden, g_attn, g_mlp, g_final, jnp.asarray(rotary_freqs()), b_q, b_k, b_v,
      w_q, w_k, w_v, k_cache, v_cache, w_o, w_gate, w_up, w_down, w_head)
    y_out, k_out, v_out, logp, lse = pl.pallas_call(
        finish_kernel,
        out_shape=(hidden, cache, cache, vector, vector),
        in_specs=[VM] * 4,
        out_specs=(HB,) * 5,
        scratch_shapes=[
            pltpu.VMEM((ROWS,), F32),
            pltpu.VMEM((ROWS,), F32),
            DMA((5,)),
        ],
        compiler_params=pltpu.CompilerParams(vmem_limit_bytes=2**20),
        name='finish',
    )(y, k_all, v_all, stats)
    shape = (ROWS, LMAX, 1, HD)
    return y_out, k_out.reshape(shape), v_out.reshape(shape), logp, lse


def solution(mesh):
    row_spec = P('dp', None)
    vec_spec = P('dp')
    cache_spec = P('dp', None, 'tp', None)
    col_spec = P(None, 'tp')
    part_spec = P('tp')
    whole_spec = P(None)
    in_specs = (row_spec, vec_spec, cache_spec, cache_spec, vec_spec, whole_spec, col_spec, part_spec, col_spec, part_spec, col_spec, part_spec, P('tp', None), whole_spec, col_spec, col_spec, P('tp', None), whole_spec, P('tp', None))
    out_specs = (row_spec, cache_spec, cache_spec, vec_spec, vec_spec)
    return jax.shard_map(local_step, mesh=mesh, in_specs=in_specs, out_specs=out_specs, check_vma=False)
```
